8 devices in a mesh: rep: 1 (over z), data: 2 (over y), model: 4 (over x, core).
Axes of the slice: x: 2, y: 2, z: 1, core: 2. Of those that a mesh axis runs over, the one named last changes fastest.
Arguments:
- x_in: bfloat16 [16, 512, 4096], P(('rep', 'data'), 'model')
- key_lens: int32 [16], P(('rep', 'data'))
- ln_gain: bfloat16 [2, 4096], P(None, 'data')
- w_in: bfloat16 [2, 4096, 33792], P(None, 'data', 'model')
- w_out_attn: bfloat16 [2, 4096, 4096], P(None, 'model', 'data')
- w_out_mlp: bfloat16 [2, 14336, 4096], P(None, 'model', 'data')
Outputs:
- output: bfloat16 [16, 512, 4096], P(('rep', 'data'), 'model')
All inputs are finite; a program needn't handle non-finite values.
Results may differ from the reference program's by a relative error of at most 0.0162603.
Values are sent between devices in bfloat16 or wider.
A program may use at most 1 GiB of HBM per device.

```python
import jax
import jax.numpy as jnp
from jax import lax

D = 4096
HEADS = 32
HEAD = 128
FF = 14336
KV_HEADS = 4
LAYERS = 2
BATCH = 16
SEQ = 512

Q_GROUP = HEADS // KV_HEADS
FF_GROUP = FF // KV_HEADS
Q_WIDTH = Q_GROUP * HEAD
FF_START = Q_WIDTH + 2 * HEAD
BLOCK_IN = FF_START + 2 * FF_GROUP
EPSILON = 1e-6
NEG_BIG = -1e30


def draw_lengths(len_key):
    drawn = jax.random.randint(len_key, (BATCH,), SEQ // 2, SEQ + 1, dtype=jnp.int32)
    return jnp.where(jnp.arange(BATCH) == 0, SEQ, drawn).astype(jnp.int32)


def setup_inputs(seed: int = 0, part: int = 0) -> dict:
    part_key = jax.random.fold_in(jax.random.key(seed), part)
    act_key, len_key = jax.random.split(part_key, 2)
    shared = jax.random.split(jax.random.key(seed + 1), 4)
    x_in = jax.random.normal(act_key, (BATCH, SEQ, D), jnp.float32).astype(jnp.bfloat16)
    key_lens = draw_lengths(len_key)
    ln_gain = (1.0 + 0.3 * jax.random.normal(shared[0], (LAYERS, D), jnp.float32)).astype(jnp.bfloat16)
    in_cols = jnp.arange(BLOCK_IN)
    in_scale = jnp.where(in_cols < Q_WIDTH + HEAD, 1.5, 1.0) * D ** -0.5
    w_in = (jax.random.normal(shared[1], (LAYERS, D, KV_HEADS, BLOCK_IN), jnp.float32) * in_scale).reshape(LAYERS, D, KV_HEADS * BLOCK_IN).astype(jnp.bfloat16)
    out_scale = (HEADS * HEAD + FF) ** -0.5
    w_out_attn = (2.0 * out_scale * jax.random.normal(shared[2], (LAYERS, HEADS * HEAD, D), jnp.float32)).astype(jnp.bfloat16)
    w_out_mlp = (out_scale * jax.random.normal(shared[3], (LAYERS, FF, D), jnp.float32)).astype(jnp.bfloat16)
    return {'x_in': x_in, 'key_lens': key_lens, 'ln_gain': ln_gain, 'w_in': w_in, 'w_out_attn': w_out_attn, 'w_out_mlp': w_out_mlp}


def layer_norm(act_in, gain_vec):
    act_f32 = act_in.astype(jnp.float32)
    row_mean = jnp.mean(act_f32, axis=-1, keepdims=True)
    centered = act_f32 - row_mean
    row_var = jnp.mean(centered * centered, axis=-1, keepdims=True)
    return (centered * lax.rsqrt(row_var + EPSILON) * gain_vec.astype(jnp.float32)).astype(jnp.bfloat16)


def mix_block(h_seq, key_len, w_in_l, w_attn_g, w_mlp_g):
    projected = jnp.dot(h_seq, w_in_l, preferred_element_type=jnp.float32).astype(jnp.bfloat16)
    projected = projected.reshape(SEQ, KV_HEADS, BLOCK_IN).astype(jnp.float32)
    queries = projected[:, :, :Q_WIDTH].reshape(SEQ, KV_HEADS, Q_GROUP, HEAD)
    key_heads = projected[:, :, Q_WIDTH:Q_WIDTH + HEAD]
    value_heads = projected[:, :, Q_WIDTH + HEAD:FF_START]
    gate_proj = projected[:, :, FF_START:FF_START + FF_GROUP]
    up_proj = projected[:, :, FF_START + FF_GROUP:]
    scores = jnp.einsum('qhgd,khd->hgqk', queries, key_heads) * HEAD ** -0.5
    positions = jnp.arange(SEQ)
    allowed = (positions[None, :] <= positions[:, None]) & (positions[None, :] < key_len)
    scores = jnp.where(allowed, scores, NEG_BIG)
    soft_probs = jax.nn.softmax(scores, axis=-1)
    attn_heads = jnp.einsum('hgqk,khd->qhgd', soft_probs, value_heads).astype(jnp.bfloat16).reshape(SEQ, KV_HEADS, Q_WIDTH)
    mlp_act = (jax.nn.silu(gate_proj) * up_proj).astype(jnp.bfloat16)
    group_part = (jnp.einsum('shr,hrd->hsd', attn_heads.astype(jnp.float32), w_attn_g) + jnp.einsum('shf,hfd->hsd', mlp_act.astype(jnp.float32), w_mlp_g)).astype(jnp.bfloat16)
    return jnp.sum(group_part.astype(jnp.float32), axis=0)


def reference(x_in, key_lens, ln_gain, w_in, w_out_attn, w_out_mlp):
    def layer_step(hidden, layer_weights):
        gain_vec, w_in_l, w_attn_l, w_mlp_l = layer_weights
        w_attn_g = w_attn_l.reshape(KV_HEADS, Q_WIDTH, D).astype(jnp.float32)
        w_mlp_g = w_mlp_l.reshape(KV_HEADS, FF_GROUP, D).astype(jnp.float32)

        def per_sequence(seq_args):
            x_seq, key_len = seq_args
            h_seq = layer_norm(x_seq, gain_vec)
            z_sum = mix_block(h_seq, key_len, w_in_l, w_attn_g, w_mlp_g)
            return (x_seq.astype(jnp.float32) + z_sum).astype(jnp.bfloat16)

        return lax.map(per_sequence, (hidden, key_lens)), None

    y_out, unused_stack = lax.scan(layer_step, x_in, (ln_gain, w_in, w_out_attn, w_out_mlp))
    return y_out
```

```python
import jax
import jax.numpy as jnp
from jax import lax
from jax.experimental import pallas as pl
from jax.experimental.pallas import tpu as pltpu
from jax.sharding import PartitionSpec as P

EPSILON = 1e-6
HEAD = 128
UNIT = 256
TILE = 512
NEG = -1e30
MESH = pl.DeviceIdType.MESH
BF = jnp.bfloat16
F32 = jnp.float32


def make_kernel(rows, seqs, d, dh, block_in, aw, ff, n_units):
    q_heads = aw // HEAD
    ff0 = aw + 2 * HEAD
    n_gu = ff // UNIT
    gate_u = ff0 // UNIT
    up_u = (ff0 + ff) // UNIT
    kv_u = aw // UNIT
    n_q = aw // TILE
    n_out = d // TILE
    n_half = n_out // 2
    pos = rows // seqs
    early = 8
    visits = 2 * early + (n_gu - early)
    kk = aw + ff
    lnr = 64
    n_ln = rows // lnr
    n_hb = n_ln // 2
    hb = 2 * lnr
    qscale = HEAD ** -0.5 * 1.4426950408889634

    def kernel(x, lens, gain, w_in, w_at, w_ml,
               y_out, a_in, a_at, a_ml, r_in, r_at, r_ml, h_all, kvb, q_b, m_b, z_b, xr, yq, yr, hid,
               big, wv, ov, xin, hst, gv, lv, qv, kvv,
               a_s, a_r, wy_s, wy_r, wc_s, wc_r, oy_s, oy_r, oc_s, oc_r, hy_s, hy_r, hx_s, hx_r, hf_s, hf_r,
               kv_s, kv_r, xz_s, xz_r, yz_s, yz_r, g_s, g_r, lg, li, lh, lo, hl, ws, os_, ai, ml_s, ad):
        rep = lax.axis_index('rep')
        y = lax.axis_index('data')
        m = lax.axis_index('model')
        xx = lax.div(m, 2)
        c = lax.rem(m, 2)
        ypeer = (rep, 1 - y, m)
        xpeer = (rep, y, lax.rem(m + 2, 4))
        cpeer = (rep, y, m + 1 - 2 * c)
        keeper = c == y
        giver = c != y

        def remote(src, dst, ss, rs, dev):
            return pltpu.make_async_remote_copy(src_ref=src, dst_ref=dst, send_sem=ss, recv_sem=rs, device_id=dev,
                                                device_id_type=MESH)

        def local(src, dst, sem):
            return pltpu.make_async_copy(src, dst, sem)

        def loop(lo_, hi_, body):
            def step(i, carry):
                body(i)
                return carry
            lax.fori_loop(lo_, hi_, step, 0)

        def ucols(u):
            return pl.ds(pl.multiple_of(u * UNIT, UNIT), UNIT)

        def tcols(t):
            return pl.ds(pl.multiple_of(t * TILE, TILE), TILE)

        def wy(l, u):
            return remote(w_in.at[l, :, ucols(u)], r_in.at[l, :, ucols(u)], wy_s.at[l, u], wy_r.at[l, u], ypeer)

        def wc(l, u):
            return remote(r_in.at[l, :, ucols(u)], r_in.at[l, :, ucols(u)], wc_s.at[l, u], wc_r.at[l, u], cpeer)

        def oy(l, t):
            return (remote(w_at.at[l, :, tcols(t)], r_at.at[l, :, tcols(t)], oy_s.at[l, t, 0], oy_r.at[l, t, 0], ypeer),
                    remote(w_ml.at[l, :, tcols(t)], r_ml.at[l, :, tcols(t)], oy_s.at[l, t, 1], oy_r.at[l, t, 1], ypeer))

        def oc(l, t):
            return (remote(r_at.at[l, :, tcols(t)], r_at.at[l, :, tcols(t)], oc_s.at[l, t, 0], oc_r.at[l, t, 0], cpeer),
                    remote(r_ml.at[l, :, tcols(t)], r_ml.at[l, :, tcols(t)], oc_s.at[l, t, 1], oc_r.at[l, t, 1], cpeer))

        def acopy(l):
            return (remote(w_in.at[l], a_in.at[l], a_s.at[l, 0], a_r.at[l, 0], cpeer),
                    remote(w_at.at[l], a_at.at[l], a_s.at[l, 1], a_r.at[l, 1], cpeer),
                    remote(w_ml.at[l], a_ml.at[l], a_s.at[l, 2], a_r.at[l, 2], cpeer))

        def hrows(b):
            return pl.ds(pl.multiple_of(b * hb, hb), hb)

        def hy(l, b):
            return remote(h_all.at[l, 0, hrows(b)], h_all.at[l, 1, hrows(b)], hy_s.at[l, b], hy_r.at[l, b], ypeer)

        def hx(l, b):
            return remote(h_all.at[l, 0, hrows(b)], h_all.at[l, 2, hrows(b)], hx_s.at[l, b], hx_r.at[l, b], xpeer)

        def hf(l):
            return remote(h_all.at[l, 1], h_all.at[l, 3], hf_s.at[l], hf_r.at[l], xpeer)

        def kvx(l):
            return remote(kvb.at[l, 0], kvb.at[l, 1], kv_s.at[l], kv_r.at[l], cpeer)

        def xz(l, t, i):
            return remote(z_b.at[l, 2 + i, :, tcols(t)], xr.at[l, i, :, tcols(t)], xz_s.at[l, t, i], xz_r.at[l, t, i], xpeer)

        def yz(l, t):
            return remote(yq.at[l, :, tcols(t)], yr.at[l, :, tcols(t)], yz_s.at[l, t], yz_r.at[l, t], ypeer)

        def issue_gu(l, j):
            wy(l, gate_u + j).start()
            wy(l, up_u + j).start()

        def issue_qkv(l):
            wy(l, kv_u).start()
            loop(0, kv_u, lambda u: wy(l, u).start())

        def issue_o(l, t):
            for cp in oy(l, t):
                cp.start()

        def arrive(l, u):
            @pl.when(keeper)
            def _():
                wy(l, u).wait_recv()
                wc(l, u).start()

            @pl.when(giver)
            def _():
                wc(l, u).wait_recv()

        def arrive_o(l, t):
            @pl.when(keeper)
            def _():
                for cp, fw in zip(oy(l, t), oc(l, t)):
                    cp.wait_recv()
                    fw.start()

            @pl.when(giver)
            def _():
                for fw in oc(l, t):
                    fw.wait_recv()

        def near_in(l, u, slot, half):
            return wv.at[slot, pl.ds(pl.multiple_of(y * dh, dh), dh), half * UNIT:(half + 1) * UNIT]

        def load_unit(l, u, slot, half):
            near = wv.at[slot, pl.ds(pl.multiple_of(y * dh, dh), dh), half * UNIT:(half + 1) * UNIT]
            far = wv.at[slot, pl.ds(pl.multiple_of((1 - y) * dh, dh), dh), half * UNIT:(half + 1) * UNIT]

            @pl.when(keeper)
            def _():
                local(w_in.at[l, :, ucols(u)], near, ws.at[slot, half]).start()

            @pl.when(giver)
            def _():
                local(a_in.at[l, :, ucols(u)], near, ws.at[slot, half]).start()

            local(r_in.at[l, :, ucols(u)], far, ws.at[slot, 2 + half]).start()

        def wait_unit(slot, half):
            near = wv.at[slot, pl.ds(pl.multiple_of(y * dh, dh), dh), half * UNIT:(half + 1) * UNIT]
            far = wv.at[slot, pl.ds(pl.multiple_of((1 - y) * dh, dh), dh), half * UNIT:(half + 1) * UNIT]
            local(r_in.at[0, :, ucols(0)], near, ws.at[slot, half]).wait()
            local(r_in.at[0, :, ucols(0)], far, ws.at[slot, 2 + half]).wait()

        def load_o(l, src_at, src_ml, t, slot):
            local(src_at.at[l, :, tcols(t)], wv.at[slot, 0:aw], ws.at[slot, 0]).start()
            local(src_ml.at[l, :, tcols(t)], wv.at[slot, aw:kk], ws.at[slot, 1]).start()

        def load_o_near(l, t, slot):
            @pl.when(keeper)
            def _():
                load_o(l, w_at, w_ml, t, slot)

            @pl.when(giver)
            def _():
                load_o(l, a_at, a_ml, t, slot)

        def wait_o(slot):
            local(r_at.at[0, :, tcols(0)], wv.at[slot, 0:aw], ws.at[slot, 0]).wait()
            local(r_ml.at[0, :, tcols(0)], wv.at[slot, aw:kk], ws.at[slot, 1]).wait()

        def lrows(r):
            return pl.ds(pl.multiple_of(r * lnr, lnr), lnr)

        def ln_phase(kind):
            l = 0 if kind == 0 else kind - 1
            ln = 1 if kind == 1 else 0
            base = hid if kind == 2 else x
            srcs = [base] if kind == 0 else [base, z_b.at[l, 0], xr.at[l, 0], yr.at[l]]

            def loads(r, slot):
                return [local(s.at[lrows(r)], xin.at[slot, i], li.at[slot, i]) for i, s in enumerate(srcs)]

            def store_h(r, slot):
                return local(big.at[0, lrows(r), 0:d], h_all.at[ln, 0, lrows(r)], lh.at[slot])

            def store_o(r, slot):
                return local(hst.at[slot], (hid if kind == 1 else y_out).at[lrows(r)], lo.at[slot])

            def send(b):
                hy(ln, b).start()
                hx(ln, b).start()

            for cp in loads(0, 0):
                cp.start()

            def block(r):
                slot = lax.rem(r, 2)

                @pl.when(r + 1 < n_ln)
                def _():
                    for cp in loads(r + 1, 1 - slot):
                        cp.start()
                for cp in loads(r, slot):
                    cp.wait()
                if kind > 0:
                    @pl.when(r >= 2)
                    def _():
                        store_o(r - 2, slot).wait()

                def sub(i):
                    rs = pl.ds(pl.multiple_of(i * 32, 32), 32)
                    v = xin[slot, 0, rs, :].astype(F32)
                    if kind > 0:
                        zs = xin[slot, 1, rs, :].astype(F32) + xin[slot, 2, rs, :].astype(F32)
                        v = (v + (zs + xin[slot, 3, rs, :].astype(F32))).astype(BF)
                        hst[slot, rs, :] = v
                        v = v.astype(F32)
                    if kind < 2:
                        mean = jnp.sum(v, axis=-1, keepdims=True) * (1.0 / d)
                        cen = v - mean
                        var = jnp.sum(cen * cen, axis=-1, keepdims=True) * (1.0 / d)
                        out = cen * lax.rsqrt(var + EPSILON) * gv[ln, 0:1, :]
                        big[0, pl.ds(pl.multiple_of(r * lnr + i * 32, 32), 32), 0:d] = out.astype(BF)
                loop(0, lnr // 32, sub)
                if kind > 0:
                    store_o(r, slot).start()
                if kind < 2:
                    store_h(r, slot).start()

                    @pl.when(r >= 1)
                    def _():
                        store_h(r - 1, 1 - slot).wait()

                    @pl.when(jnp.logical_and(r >= 2, lax.rem(r, 2) == 0))
                    def _():
                        send(lax.div(r, 2) - 1)
            loop(0, n_ln, block)
            if kind > 0:
                store_o(n_ln - 2, 0).wait()
                store_o(n_ln - 1, 1).wait()
            if kind < 2:
                store_h(n_ln - 1, 1).wait()
                send(n_hb - 1)

        barrier = pltpu.get_barrier_semaphore()
        for dev in (ypeer, xpeer, cpeer):
            pl.semaphore_signal(barrier, inc=1, device_id=dev, device_id_type=MESH)
        pl.semaphore_wait(barrier, 3)

        def gain_y():
            half = gv.at[:, :, pl.ds(pl.multiple_of(y * dh, dh), dh)]
            return remote(gain, half, g_s.at[0], g_r.at[0], ypeer)

        def lens_y():
            return remote(lens, lv.at[1], g_s.at[1], g_r.at[1], ypeer)

        def gain_l():
            return local(gain, gv.at[:, :, pl.ds(pl.multiple_of(y * dh, dh), dh)], lg.at[0])

        def lens_l():
            return local(lens, lv.at[0], lg.at[1])

        gain_y().start()
        lens_y().start()
        gain_l().start()
        lens_l().start()

        @pl.when(keeper)
        def _():
            for l in range(2):
                for cp in acopy(l):
                    cp.start()

        @pl.when(giver)
        def _():
            issue_gu(0, 0)
        gain_l().wait()
        lens_l().wait()
        gain_y().wait()
        lens_y().wait()
        ln_phase(0)

        @pl.when(giver)
        def _():
            loop(1, n_gu, lambda j: issue_gu(0, j))
            issue_qkv(0)
            loop(0, n_half, lambda t: issue_o(0, t))

        def layer(l):
            @pl.when(giver)
            def _():
                for cp in acopy(l):
                    cp.wait_recv()

            def h_load(s):
                return local(h_all.at[l, s], big.at[s, :, 0:d], hl.at[s])

            loop(0, n_hb, lambda b: hy(l, b).wait_recv())
            hf(l).start()
            h_load(1).start()
            loop(0, n_hb, lambda b: hx(l, b).wait_recv())
            h_load(2).start()
            arrive(l, gate_u)
            arrive(l, up_u)
            load_unit(l, gate_u, 0, 0)
            load_unit(l, up_u, 0, 1)
            h_load(1).wait()
            h_load(2).wait()

            def m_store(s, j):
                return local(ov.at[s, :, 0:UNIT], m_b.at[s, :, ucols(j)], os_.at[s])

            def visit(v):
                slot = lax.rem(v, 2)
                wait_unit(slot, 0)
                wait_unit(slot, 1)
                blk = lax.div(v, early)
                j = v - early * lax.div(lax.min(blk, 2) + 1, 2)
                s_lo = 3 * lax.rem(lax.min(blk, 2), 2)
                s_hi = 3 + lax.div(lax.min(blk, 2) + 1, 2)
                s_pf = s_lo + lax.div(s_hi - s_lo, 2)

                @pl.when(v == early)
                def _():
                    hf(l).wait_recv()
                    h_load(3).start()
                    h_load(3).wait()

                def shard(s):
                    @pl.when(s == s_pf)
                    def _():
                        nv = v + 1
                        nj = nv - early * lax.div(lax.min(lax.div(nv, early), 2) + 1, 2)

                        @pl.when(jnp.logical_and(lax.div(nv, early) != 1, nv < visits))
                        def _():
                            arrive(l, gate_u + nj)
                            arrive(l, up_u + nj)

                        @pl.when(nv < visits)
                        def _():
                            load_unit(l, gate_u + nj, 1 - slot, 0)
                            load_unit(l, up_u + nj, 1 - slot, 1)

                        @pl.when(nv == visits)
                        def _():
                            arrive(l, kv_u)
                            load_unit(l, kv_u, visits % 2, 0)

                    @pl.when(v != early * lax.div(s, 3))
                    def _():
                        m_store(s, 0).wait()
                    acc = jnp.dot(big[s, :, 0:d], wv[slot, 0:d, :], preferred_element_type=F32)
                    g = acc[:, :UNIT].astype(BF).astype(F32)
                    u = acc[:, UNIT:].astype(BF).astype(F32)
                    ov[s, :, 0:UNIT] = (g * jax.nn.sigmoid(g) * u).astype(BF)
                    m_store(s, j).start()
                loop(s_lo, s_hi, shard)
            loop(0, visits, visit)

            kslot = visits % 2
            wait_unit(kslot, 0)

            def kv_store(s):
                return local(ov.at[s, :, 0:UNIT], kvb.at[l, 0, s], os_.at[s])

            def kv_shard(s):
                @pl.when(s == 2)
                def _():
                    for u in range(2):
                        arrive(l, u)
                        load_unit(l, u, 1 - kslot, u)
                m_store(s, 0).wait()
                acc = jnp.dot(big[s, :, 0:d], wv[kslot, 0:d, 0:UNIT], preferred_element_type=F32)
                ov[s, :, 0:UNIT] = acc.astype(BF)
                kv_store(s).start()
            loop(0, 4, kv_shard)

            def q_store(s, t):
                return local(ov.at[s], q_b.at[s, :, tcols(t)], os_.at[s])

            def q_tile(t):
                slot = lax.rem(t + 1 - kslot, 2)
                wait_unit(slot, 0)
                wait_unit(slot, 1)

                def shard(s):
                    @pl.when(jnp.logical_and(s == 2, t + 1 < n_q))
                    def _():
                        for i in range(2):
                            arrive(l, 2 * (t + 1) + i)
                            load_unit(l, 2 * (t + 1) + i, 1 - slot, i)

                    @pl.when(t == 0)
                    def _():
                        kv_store(s).wait()

                    @pl.when(t > 0)
                    def _():
                        q_store(s, 0).wait()
                    acc = jnp.dot(big[s, :, 0:d], wv[slot, 0:d, :], preferred_element_type=F32)
                    ov[s] = acc.astype(BF)
                    q_store(s, t).start()
                loop(0, 4, shard)

                @pl.when(t == 0)
                def _():
                    kvx(l).start()
            loop(0, n_q, q_tile)
            loop(0, 4, lambda s: q_store(s, 0).wait())

            def m_load(s):
                return local(m_b.at[s], big.at[s, :, aw:kk], ml_s.at[s])
            loop(0, 4, lambda s: m_load(s).start())
            oslot = (1 - kslot + n_q) % 2
            load_o_near(l, 0, oslot)
            kvx(l).wait_recv()

            def at_loads(i, slot):
                a = lax.div(i, seqs)
                b = lax.rem(i, seqs)
                rs = pl.ds(pl.multiple_of(b * pos, pos), pos)

                def at(quarter):
                    return kvv.at[slot, pl.ds(pl.multiple_of(quarter * pos, pos), pos)]
                return (local(q_b.at[a, rs], qv.at[slot, xx], ai.at[slot, 0]),
                        local(q_b.at[2 + a, rs], qv.at[slot, 1 - xx], ai.at[slot, 1]),
                        local(kvb.at[l, 0, a, rs], at(2 * xx + c), ai.at[slot, 2]),
                        local(kvb.at[l, 0, 2 + a, rs], at(2 * (1 - xx) + c), ai.at[slot, 3]),
                        local(kvb.at[l, 1, a, rs], at(2 * xx + 1 - c), ai.at[slot, 4]),
                        local(kvb.at[l, 1, 2 + a, rs], at(2 * (1 - xx) + 1 - c), ai.at[slot, 5]))

            for cp in at_loads(0, 0):
                cp.start()

            def seq(i):
                slot = lax.rem(i, 2)
                a = lax.div(i, seqs)
                b = lax.rem(i, seqs)

                @pl.when(i + 1 < 2 * seqs)
                def _():
                    for cp in at_loads(i + 1, 1 - slot):
                        cp.start()
                for cp in at_loads(i, slot):
                    cp.wait()
                row = pl.ds(pl.multiple_of(b * pos, pos), pos)
                for blk in range(2):
                    nk = 2 * pos * (blk + 1)
                    qpos = lax.broadcasted_iota(jnp.int32, (pos, nk), 0) + (2 * blk + c) * pos
                    kpos = lax.broadcasted_iota(jnp.int32, (pos, nk), 1)
                    ok = jnp.logical_and(kpos <= qpos, kpos < lv[a, pl.ds(b, 1), 0:nk])
                    keys = kvv[slot, 0:nk, 0:HEAD]
                    vals = kvv[slot, 0:nk, HEAD:2 * HEAD]
                    sh = a + 2 * (blk + xx - 2 * blk * xx)
                    for hd in range(q_heads):
                        cs = slice(hd * HEAD, (hd + 1) * HEAD)
                        s = lax.dot_general(qv[slot, blk, :, cs], keys, (((1,), (1,)), ((), ())),
                                            preferred_element_type=F32) * qscale
                        s = jnp.where(ok, s, NEG)
                        e = jnp.exp2(s - jnp.max(s, axis=-1, keepdims=True))
                        den = jnp.sum(e, axis=-1, keepdims=True)
                        o = jnp.dot(e.astype(BF), vals, preferred_element_type=F32)
                        big[sh, row, cs] = (o / den).astype(BF)
            loop(0, 2 * seqs, seq)

            @pl.when(jnp.logical_and(giver, l == 0))
            def _():
                loop(0, 2, lambda j: issue_gu(1, j))
            loop(0, 4, lambda s: m_load(s).wait())

            def tau(k):
                return lax.rem(y + lax.div(k, n_half), 2) * n_half + lax.rem(k, n_half)

            def z_store(s, t):
                return local(ov.at[s], z_b.at[l, s, :, tcols(t)], os_.at[s])

            def out_tile(k):
                slot = lax.rem(k + oslot, 2)
                t = tau(k)
                wait_o(slot)

                def shard(si):
                    s = lax.rem(si + 2, 4)

                    @pl.when(jnp.logical_and(si == 2, k + 1 < n_half))
                    def _():
                        load_o_near(l, k + 1, 1 - slot)

                    @pl.when(jnp.logical_and(si == 2, jnp.logical_and(k + 1 >= n_half, k + 1 < n_out)))
                    def _():
                        arrive_o(l, k + 1 - n_half)
                        load_o(l, r_at, r_ml, k + 1 - n_half, 1 - slot)

                    @pl.when(jnp.logical_and(si >= 2, k > 0))
                    def _():
                        z_store(s, t).wait()

                    @pl.when(jnp.logical_and(si >= 1, si < 3))
                    def _():
                        z_store(si + 1, t).wait()
                        xz(l, t, si - 1).start()
                    acc = jnp.dot(big[s], wv[slot], preferred_element_type=F32)
                    ov[s] = acc.astype(BF)
                    z_store(s, t).start()
                loop(0, 4, shard)
            loop(0, n_out, out_tile)
            loop(0, 2, lambda s: z_store(s, 0).wait())

            def add_tile(k):
                t = tau(k)
                xz(l, t, 0).wait_recv()
                xz(l, t, 1).wait_recv()
                lhs = local(z_b.at[l, 1, :, tcols(t)], ov.at[0], ad.at[0])
                rhs = local(xr.at[l, 1, :, tcols(t)], ov.at[1], ad.at[1])
                lhs.start()
                rhs.start()
                lhs.wait()
                rhs.wait()

                def sub(i):
                    rs = pl.ds(pl.multiple_of(i * 128, 128), 128)
                    ov[0, rs, :] = (ov[0, rs, :].astype(F32) + ov[1, rs, :].astype(F32)).astype(BF)
                loop(0, rows // 128, sub)
                out = local(ov.at[0], yq.at[l, :, tcols(t)], ad.at[2])
                out.start()
                out.wait()
                yz(l, t).start()

                @pl.when(jnp.logical_and(giver, jnp.logical_and(l == 0, k >= 5)))
                def _():
                    issue_gu(1, k - 3)
            loop(0, n_out, add_tile)
            loop(0, n_out, lambda t: yz(l, t).wait_recv())

            @pl.when(l == 0)
            def _():
                ln_phase(1)

                @pl.when(giver)
                def _():
                    loop(5, n_gu, lambda j: issue_gu(1, j))
                    issue_qkv(1)
                    loop(0, n_half, lambda t: issue_o(1, t))

            @pl.when(l == 1)
            def _():
                ln_phase(2)

            def sent_h(b):
                hy(l, b).wait_send()
                hx(l, b).wait_send()
            loop(0, n_hb, sent_h)
            hf(l).wait_send()
            kvx(l).wait_send()

            def sent_z(t):
                xz(l, t, 0).wait_send()
                xz(l, t, 1).wait_send()
                yz(l, t).wait_send()
            loop(0, n_out, sent_z)

            @pl.when(giver)
            def _():
                loop(0, n_units, lambda u: wy(l, u).wait_send())

                def sent_o(t):
                    for cp in oy(l, t):
                        cp.wait_send()
                loop(0, n_half, sent_o)

            @pl.when(keeper)
            def _():
                loop(0, n_units, lambda u: wc(l, u).wait_send())

                def sent_o(t):
                    for cp in oc(l, t):
                        cp.wait_send()
                loop(0, n_half, sent_o)
                for cp in acopy(l):
                    cp.wait_send()
        loop(0, 2, layer)

    return kernel


def solution(mesh):
    batch_axes = ('rep', 'data')

    def device_step(x_loc, len_loc, gain_loc, w_in_loc, w_attn_loc, w_mlp_loc):
        seqs, pos, d = x_loc.shape
        rows = seqs * pos
        layers, dh, block_in = w_in_loc.shape
        aw = w_attn_loc.shape[1]
        ff = w_mlp_loc.shape[1]
        n_units = block_in // UNIT
        n_out = d // TILE
        kk = aw + ff
        seq_len = pos * mesh.shape['model']
        lens = jnp.broadcast_to(len_loc[:, None], (seqs, seq_len)).astype(jnp.int32)
        gain = jnp.broadcast_to(gain_loc.astype(F32)[:, None, :], (layers, 8, dh))

        def buf(*shape):
            return jax.ShapeDtypeStruct(shape, BF)

        outs = [buf(rows, d), buf(layers, dh, block_in), buf(layers, aw, dh), buf(layers, ff, dh),
                buf(layers, dh, block_in), buf(layers, aw, dh), buf(layers, ff, dh),
                buf(layers, 4, rows, d), buf(layers, 2, 4, rows, 2 * HEAD), buf(4, rows, aw), buf(4, rows, ff),
                buf(layers, 4, rows, d), buf(layers, 2, rows, d), buf(layers, rows, d), buf(layers, rows, d), buf(rows, d)]
        dma = pltpu.SemaphoreType.DMA
        n_hb = rows // 128
        scratch = [pltpu.VMEM((4, rows, kk), BF), pltpu.VMEM((2, kk, TILE), BF), pltpu.VMEM((4, rows, TILE), BF),
                   pltpu.VMEM((2, 4, 64, d), BF), pltpu.VMEM((2, 64, d), BF), pltpu.VMEM((layers, 8, d), F32),
                   pltpu.VMEM((2, seqs, seq_len), jnp.int32), pltpu.VMEM((2, 2, pos, aw), BF),
                   pltpu.VMEM((2, seq_len, 2 * HEAD), BF),
                   dma((layers, 3)), dma((layers, 3)),
                   dma((layers, n_units)), dma((layers, n_units)), dma((layers, n_units)), dma((layers, n_units)),
                   dma((layers, n_out // 2, 2)), dma((layers, n_out // 2, 2)),
                   dma((layers, n_out // 2, 2)), dma((layers, n_out // 2, 2)),
                   dma((layers, n_hb)), dma((layers, n_hb)), dma((layers, n_hb)), dma((layers, n_hb)),
                   dma((layers,)), dma((layers,)), dma((layers,)), dma((layers,)),
                   dma((layers, n_out, 2)), dma((layers, n_out, 2)), dma((layers, n_out)), dma((layers, n_out)),
                   dma((2,)), dma((2,)), dma((2,)), dma((2, 4)), dma((2,)), dma((2,)), dma((4,)), dma((2, 4)), dma((4,)),
                   dma((2, 6)), dma((4,)), dma((3,))]
        hbm = pl.BlockSpec(memory_space=pl.ANY)
        kernel = make_kernel(rows, seqs, d, dh, block_in, aw, ff, n_units)
        got = pl.pallas_call(
            kernel, out_shape=outs, in_specs=[hbm] * 6, out_specs=[hbm] * len(outs), scratch_shapes=scratch, name='two_layers',
            compiler_params=pltpu.CompilerParams(collective_id=0, has_side_effects=True, vmem_limit_bytes=67_000_000),
        )(x_loc.reshape(rows, d), lens, gain, w_in_loc, w_attn_loc, w_mlp_loc)
        return got[0].reshape(seqs, pos, d)

    return jax.shard_map(device_step, mesh=mesh,
                         in_specs=(P(batch_axes, 'model', None), P(batch_axes), P(None, 'data'), P(None, 'data', 'model'),
                                   P(None, 'model', 'data'), P(None, 'model', 'data')),
                         out_specs=P(batch_axes, 'model', None), check_vma=False)
```

```python
import jax
import jax.numpy as jnp
from jax import lax
from jax.experimental import pallas as pl
from jax.experimental.pallas import tpu as pltpu
from jax.sharding import PartitionSpec as P

EPSILON = 1e-6
HEAD = 128
UNIT = 256
TILE = 512
SOFT = 32
NEG = -1e30
MESH = pl.DeviceIdType.MESH
BF = jnp.bfloat16
F32 = jnp.float32


def make_kernel(rows, seqs, d, dh, block_in, aw, ff, n_units):
    q_heads = aw // HEAD
    ff0 = aw + 2 * HEAD
    n_gu = ff // UNIT
    gate_u = ff0 // UNIT
    up_u = (ff0 + ff) // UNIT
    kv_u = aw // UNIT
    n_q = aw // TILE
    n_out = d // TILE
    n_half = n_out // 2
    pos = rows // seqs
    early0, early1 = 8, 11
    kk = aw + ff
    lnr = 64
    n_ln = rows // lnr
    n_hb = n_ln // 2
    hb = 2 * lnr
    qscale = HEAD ** -0.5 * 1.4426950408889634

    def kernel(x, lens, gain, w_in, w_at, w_ml,
               y_out, a_in, a_at, a_ml, r_in, r_at, r_ml, h_all, kvb, q_b, m_b, z_b, xr, sq, ym, yr, hid,
               big, wv, ov, ab, xin, hst, gv, lv, qv, kvv, sv,
               a_s, a_r, wy_s, wy_r, wc_s, wc_r, oy_s, oy_r, oc_s, oc_r, hy_s, hy_r, hx_s, hx_r, hf_s, hf_r,
               kv_s, kv_r, xz_s, xz_r, yz_s, yz_r, y3_s, y3_r, g_s, g_r, lg, li, lh, lo, hl, ws, os_, ai, ml_s, ad):
        rep = lax.axis_index('rep')
        y = lax.axis_index('data')
        m = lax.axis_index('model')
        xx = lax.div(m, 2)
        c = lax.rem(m, 2)
        ypeer = (rep, 1 - y, m)
        xpeer = (rep, y, lax.rem(m + 2, 4))
        cpeer = (rep, y, m + 1 - 2 * c)
        keeper = c == y
        giver = c != y

        def remote(src, dst, ss, rs, dev):
            return pltpu.make_async_remote_copy(src_ref=src, dst_ref=dst, send_sem=ss, recv_sem=rs, device_id=dev,
                                                device_id_type=MESH)

        def local(src, dst, sem):
            return pltpu.make_async_copy(src, dst, sem)

        def loop(lo_, hi_, body):
            def step(i, carry):
                body(i)
                return carry
            lax.fori_loop(lo_, hi_, step, 0)

        def ucols(u):
            return pl.ds(pl.multiple_of(u * UNIT, UNIT), UNIT)

        def tcols(t):
            return pl.ds(pl.multiple_of(t * TILE, TILE), TILE)

        def wy(l, u):
            return remote(w_in.at[l, :, ucols(u)], r_in.at[l, :, ucols(u)], wy_s.at[l, u], wy_r.at[l, u], ypeer)

        def wc(l, u):
            return remote(r_in.at[l, :, ucols(u)], r_in.at[l, :, ucols(u)], wc_s.at[l, u], wc_r.at[l, u], cpeer)

        def oy(l, t):
            return (remote(w_at.at[l, :, tcols(t)], r_at.at[l, :, tcols(t)], oy_s.at[l, t, 0], oy_r.at[l, t, 0], ypeer),
                    remote(w_ml.at[l, :, tcols(t)], r_ml.at[l, :, tcols(t)], oy_s.at[l, t, 1], oy_r.at[l, t, 1], ypeer))

        def oc(l, t):
            return (remote(r_at.at[l, :, tcols(t)], r_at.at[l, :, tcols(t)], oc_s.at[l, t, 0], oc_r.at[l, t, 0], cpeer),
                    remote(r_ml.at[l, :, tcols(t)], r_ml.at[l, :, tcols(t)], oc_s.at[l, t, 1], oc_r.at[l, t, 1], cpeer))

        def acopy(l):
            return (remote(w_in.at[l], a_in.at[l], a_s.at[l, 0], a_r.at[l, 0], cpeer),
                    remote(w_at.at[l], a_at.at[l], a_s.at[l, 1], a_r.at[l, 1], cpeer),
                    remote(w_ml.at[l], a_ml.at[l], a_s.at[l, 2], a_r.at[l, 2], cpeer))

        def hrows(b):
            return pl.ds(pl.multiple_of(b * hb, hb), hb)

        def hy(l, b):
            return remote(h_all.at[l, 0, hrows(b)], h_all.at[l, 1, hrows(b)], hy_s.at[l, b], hy_r.at[l, b], ypeer)

        def hx(l, b):
            return remote(h_all.at[l, 0, hrows(b)], h_all.at[l, 2, hrows(b)], hx_s.at[l, b], hx_r.at[l, b], xpeer)

        def hf(l):
            return remote(h_all.at[l, 1], h_all.at[l, 3], hf_s.at[l], hf_r.at[l], xpeer)

        def kvx(l):
            return remote(kvb.at[l, 0], kvb.at[l, 1], kv_s.at[l], kv_r.at[l], cpeer)

        def xz(l, t, i):
            return remote(z_b.at[l, 2 + i, :, tcols(t)], xr.at[l, i, :, tcols(t)], xz_s.at[l, t, i], xz_r.at[l, t, i], xpeer)

        def yz(l, t):
            return remote(sq.at[l, :, tcols(t)], yr.at[l, :, tcols(t)], yz_s.at[l, t], yz_r.at[l, t], ypeer)

        def yz_first(l, t):
            return remote(z_b.at[l, 1, :, tcols(t)], yr.at[l, :, tcols(t)], yz_s.at[l, t], yz_r.at[l, t], ypeer)

        def yz_pass(l, t):
            return remote(z_b.at[l, 3, :, tcols(t)], ym.at[:, tcols(t)], y3_s.at[t], y3_r.at[t], ypeer)

        def xz_last(l, t):
            return remote(sq.at[l, :, tcols(t)], xr.at[l, 0, :, tcols(t)], xz_s.at[l, t, 0], xz_r.at[l, t, 0], xpeer)

        def y_goes_first(l, t):
            return jnp.logical_and(l == 1, lax.rem(t, n_half) == n_half - 1)

        def issue_gu(l, j):
            wy(l, gate_u + j).start()
            wy(l, up_u + j).start()

        def issue_qkv(l):
            wy(l, kv_u).start()
            loop(0, kv_u, lambda u: wy(l, u).start())

        def issue_o(l, t):
            for cp in oy(l, t):
                cp.start()

        def arrive(l, u):
            @pl.when(keeper)
            def _():
                wy(l, u).wait_recv()
                wc(l, u).start()

            @pl.when(giver)
            def _():
                wc(l, u).wait_recv()

        def arrive_o(l, t):
            @pl.when(keeper)
            def _():
                for cp, fw in zip(oy(l, t), oc(l, t)):
                    cp.wait_recv()
                    fw.start()

            @pl.when(giver)
            def _():
                for fw in oc(l, t):
                    fw.wait_recv()

        def near_in(l, u, slot, half):
            return wv.at[slot, pl.ds(pl.multiple_of(y * dh, dh), dh), half * UNIT:(half + 1) * UNIT]

        def load_unit(l, u, slot, half):
            near = wv.at[slot, pl.ds(pl.multiple_of(y * dh, dh), dh), half * UNIT:(half + 1) * UNIT]
            far = wv.at[slot, pl.ds(pl.multiple_of((1 - y) * dh, dh), dh), half * UNIT:(half + 1) * UNIT]

            @pl.when(keeper)
            def _():
                local(w_in.at[l, :, ucols(u)], near, ws.at[slot, half]).start()

            @pl.when(giver)
            def _():
                local(a_in.at[l, :, ucols(u)], near, ws.at[slot, half]).start()

            local(r_in.at[l, :, ucols(u)], far, ws.at[slot, 2 + half]).start()

        def wait_unit(slot, half):
            near = wv.at[slot, pl.ds(pl.multiple_of(y * dh, dh), dh), half * UNIT:(half + 1) * UNIT]
            far = wv.at[slot, pl.ds(pl.multiple_of((1 - y) * dh, dh), dh), half * UNIT:(half + 1) * UNIT]
            local(r_in.at[0, :, ucols(0)], near, ws.at[slot, half]).wait()
            local(r_in.at[0, :, ucols(0)], far, ws.at[slot, 2 + half]).wait()

        def load_o(l, src_at, src_ml, t, slot):
            local(src_at.at[l, :, tcols(t)], wv.at[slot, 0:aw], ws.at[slot, 0]).start()
            local(src_ml.at[l, :, tcols(t)], wv.at[slot, aw:kk], ws.at[slot, 1]).start()

        def load_o_near(l, t, slot):
            @pl.when(keeper)
            def _():
                load_o(l, w_at, w_ml, t, slot)

            @pl.when(giver)
            def _():
                load_o(l, a_at, a_ml, t, slot)

        def wait_o(slot):
            local(r_at.at[0, :, tcols(0)], wv.at[slot, 0:aw], ws.at[slot, 0]).wait()
            local(r_ml.at[0, :, tcols(0)], wv.at[slot, aw:kk], ws.at[slot, 1]).wait()

        def lrows(r):
            return pl.ds(pl.multiple_of(r * lnr, lnr), lnr)

        def ln_phase(kind):
            ln = kind
            srcs = [x, z_b.at[0, 0], xr.at[0, 0], yr.at[0]] if kind else [x]

            def loads(r, slot):
                return [local(s.at[lrows(r)], xin.at[slot, i], li.at[slot, i]) for i, s in enumerate(srcs)]

            def store_h(r, slot):
                return local(big.at[0, lrows(r), 0:d], h_all.at[ln, 0, lrows(r)], lh.at[slot])

            def store_o(r, slot):
                return local(hst.at[slot], hid.at[lrows(r)], lo.at[slot])

            def send(b):
                hy(ln, b).start()
                hx(ln, b).start()

            for cp in loads(0, 0):
                cp.start()

            def block(r):
                slot = lax.rem(r, 2)

                @pl.when(r + 1 < n_ln)
                def _():
                    for cp in loads(r + 1, 1 - slot):
                        cp.start()
                for cp in loads(r, slot):
                    cp.wait()
                if kind > 0:
                    @pl.when(r >= 2)
                    def _():
                        store_o(r - 2, slot).wait()

                def sub(i):
                    rs = pl.ds(pl.multiple_of(i * 32, 32), 32)
                    v = xin[slot, 0, rs, :].astype(F32)
                    if kind > 0:
                        zs = xin[slot, 1, rs, :].astype(F32) + xin[slot, 2, rs, :].astype(F32)
                        v = (v + (zs + xin[slot, 3, rs, :].astype(F32))).astype(BF)
                        hst[slot, rs, :] = v
                        v = v.astype(F32)
                    if True:
                        mean = jnp.sum(v, axis=-1, keepdims=True) * (1.0 / d)
                        cen = v - mean
                        var = jnp.sum(cen * cen, axis=-1, keepdims=True) * (1.0 / d)
                        out = cen * lax.rsqrt(var + EPSILON) * gv[ln, 0:1, :]
                        big[0, pl.ds(pl.multiple_of(r * lnr + i * 32, 32), 32), 0:d] = out.astype(BF)
                loop(0, lnr // 32, sub)
                if kind > 0:
                    store_o(r, slot).start()
                if True:
                    store_h(r, slot).start()

                    @pl.when(r >= 1)
                    def _():
                        store_h(r - 1, 1 - slot).wait()

                    @pl.when(jnp.logical_and(r >= 2, lax.rem(r, 2) == 0))
                    def _():
                        send(lax.div(r, 2) - 1)
            loop(0, n_ln, block)
            if kind > 0:
                store_o(n_ln - 2, 0).wait()
                store_o(n_ln - 1, 1).wait()
            store_h(n_ln - 1, 1).wait()
            send(n_hb - 1)

        barrier = pltpu.get_barrier_semaphore()
        for dev in (ypeer, xpeer, cpeer):
            pl.semaphore_signal(barrier, inc=1, device_id=dev, device_id_type=MESH)
        pl.semaphore_wait(barrier, 3)

        def gain_y():
            half = gv.at[:, :, pl.ds(pl.multiple_of(y * dh, dh), dh)]
            return remote(gain, half, g_s.at[0], g_r.at[0], ypeer)

        def lens_y():
            return remote(lens, lv.at[1], g_s.at[1], g_r.at[1], ypeer)

        def gain_l():
            return local(gain, gv.at[:, :, pl.ds(pl.multiple_of(y * dh, dh), dh)], lg.at[0])

        def lens_l():
            return local(lens, lv.at[0], lg.at[1])

        gain_y().start()
        lens_y().start()
        gain_l().start()
        lens_l().start()

        @pl.when(keeper)
        def _():
            for l in range(2):
                for cp in acopy(l):
                    cp.start()

        @pl.when(giver)
        def _():
            issue_gu(0, 0)
        gain_l().wait()
        lens_l().wait()
        gain_y().wait()
        lens_y().wait()
        ln_phase(0)

        @pl.when(giver)
        def _():
            loop(1, n_gu, lambda j: issue_gu(0, j))
            issue_qkv(0)
            loop(0, n_half, lambda t: issue_o(0, t))

        def layer(l):
            @pl.when(giver)
            def _():
                for cp in acopy(l):
                    cp.wait_recv()

            def h_load(s):
                return local(h_all.at[l, s], big.at[s, :, 0:d], hl.at[s])

            loop(0, n_hb, lambda b: hy(l, b).wait_recv())
            hf(l).start()
            h_load(1).start()
            loop(0, n_hb, lambda b: hx(l, b).wait_recv())
            h_load(2).start()
            arrive(l, gate_u)
            arrive(l, up_u)
            load_unit(l, gate_u, 0, 0)
            load_unit(l, up_u, 0, 1)
            h_load(1).wait()
            h_load(2).wait()

            def m_store(s, j):
                return local(ov.at[s, :, 0:UNIT], m_b.at[s, :, ucols(j)], os_.at[s])

            early = early0 + (early1 - early0) * l
            visits = n_gu + early

            def visit(v):
                slot = lax.rem(v, 2)
                wait_unit(slot, 0)
                wait_unit(slot, 1)
                blk = lax.div(v, early)
                j = v - early * lax.div(lax.min(blk, 2) + 1, 2)
                s_lo = 3 * lax.rem(lax.min(blk, 2), 2)
                s_hi = 3 + lax.div(lax.min(blk, 2) + 1, 2)
                s_pf = s_lo + lax.div(s_hi - s_lo, 2)

                @pl.when(v == early)
                def _():
                    hf(l).wait_recv()
                    h_load(3).start()
                    h_load(3).wait()

                def shard(s):
                    @pl.when(s == s_pf)
                    def _():
                        nv = v + 1
                        nj = nv - early * lax.div(lax.min(lax.div(nv, early), 2) + 1, 2)

                        @pl.when(jnp.logical_and(lax.div(nv, early) != 1, nv < visits))
                        def _():
                            arrive(l, gate_u + nj)
                            arrive(l, up_u + nj)

                        @pl.when(nv < visits)
                        def _():
                            load_unit(l, gate_u + nj, 1 - slot, 0)
                            load_unit(l, up_u + nj, 1 - slot, 1)

                        @pl.when(nv == visits)
                        def _():
                            arrive(l, kv_u)
                            load_unit(l, kv_u, lax.rem(visits, 2), 0)

                    @pl.when(v != early * lax.div(s, 3))
                    def _():
                        m_store(s, 0).wait()
                    acc = jnp.dot(big[s, :, 0:d], wv[slot, 0:d, :], preferred_element_type=F32)
                    g = acc[:, :UNIT].astype(BF).astype(F32)
                    u = acc[:, UNIT:].astype(BF).astype(F32)
                    ov[s, :, 0:UNIT] = (g * jax.nn.sigmoid(g) * u).astype(BF)
                    m_store(s, j).start()
                loop(s_lo, s_hi, shard)
            loop(0, visits, visit)

            kslot = lax.rem(n_gu + early, 2)
            wait_unit(kslot, 0)

            def kv_store(s):
                return local(ov.at[s, :, 0:UNIT], kvb.at[l, 0, s], os_.at[s])

            def kv_shard(s):
                @pl.when(s == 2)
                def _():
                    for u in range(2):
                        arrive(l, u)
                        load_unit(l, u, 1 - kslot, u)
                m_store(s, 0).wait()
                acc = jnp.dot(big[s, :, 0:d], wv[kslot, 0:d, 0:UNIT], preferred_element_type=F32)
                ov[s, :, 0:UNIT] = acc.astype(BF)
                kv_store(s).start()
            loop(0, 4, kv_shard)

            def q_store(s, t):
                return local(ov.at[s], q_b.at[s, :, tcols(t)], os_.at[s])

            def q_tile(t):
                slot = lax.rem(t + 1 + kslot, 2)
                wait_unit(slot, 0)
                wait_unit(slot, 1)

                def shard(s):
                    @pl.when(jnp.logical_and(s == 2, t + 1 < n_q))
                    def _():
                        for i in range(2):
                            arrive(l, 2 * (t + 1) + i)
                            load_unit(l, 2 * (t + 1) + i, 1 - slot, i)

                    @pl.when(t == 0)
                    def _():
                        kv_store(s).wait()

                    @pl.when(t > 0)
                    def _():
                        q_store(s, 0).wait()
                    acc = jnp.dot(big[s, :, 0:d], wv[slot, 0:d, :], preferred_element_type=F32)
                    ov[s] = acc.astype(BF)
                    q_store(s, t).start()
                loop(0, 4, shard)

                @pl.when(t == 0)
                def _():
                    kvx(l).start()
            loop(0, n_q, q_tile)
            loop(0, 4, lambda s: q_store(s, 0).wait())

            def m_load(s):
                return local(m_b.at[s], big.at[s, :, aw:kk], ml_s.at[s])
            loop(0, 4, lambda s: m_load(s).start())
            oslot = lax.rem(1 + kslot + n_q, 2)
            load_o_near(l, 0, oslot)
            kvx(l).wait_recv()

            def at_loads(i, slot):
                a = lax.div(i, seqs)
                b = lax.rem(i, seqs)
                rs = pl.ds(pl.multiple_of(b * pos, pos), pos)

                def at(quarter):
                    return kvv.at[slot, pl.ds(pl.multiple_of(quarter * pos, pos), pos)]
                return (local(q_b.at[a, rs], qv.at[slot, xx], ai.at[slot, 0]),
                        local(q_b.at[2 + a, rs], qv.at[slot, 1 - xx], ai.at[slot, 1]),
                        local(kvb.at[l, 0, a, rs], at(2 * xx + c), ai.at[slot, 2]),
                        local(kvb.at[l, 0, 2 + a, rs], at(2 * (1 - xx) + c), ai.at[slot, 3]),
                        local(kvb.at[l, 1, a, rs], at(2 * xx + 1 - c), ai.at[slot, 4]),
                        local(kvb.at[l, 1, 2 + a, rs], at(2 * (1 - xx) + 1 - c), ai.at[slot, 5]))

            for cp in at_loads(0, 0):
                cp.start()

            def seq(i):
                slot = lax.rem(i, 2)
                a = lax.div(i, seqs)
                b = lax.rem(i, seqs)

                @pl.when(i + 1 < 2 * seqs)
                def _():
                    for cp in at_loads(i + 1, 1 - slot):
                        cp.start()
                for cp in at_loads(i, slot):
                    cp.wait()
                row = pl.ds(pl.multiple_of(b * pos, pos), pos)
                for blk in range(2):
                    nk = 2 * pos * (blk + 1)
                    keys = kvv[slot, 0:nk, 0:HEAD]
                    vals = kvv[slot, 0:nk, HEAD:2 * HEAD]
                    sh = a + 2 * (blk + xx - 2 * blk * xx)
                    q_all = jnp.concatenate([qv[slot, blk, :, hd * HEAD:(hd + 1) * HEAD] for hd in range(q_heads)], axis=0)
                    sv[:, 0:nk] = lax.dot_general(q_all, keys, (((1,), (1,)), ((), ())), preferred_element_type=F32)

                    def head(hd):
                        for part in range(pos // SOFT):
                            r0 = part * SOFT
                            rs = slice(hd * pos + r0, hd * pos + r0 + SOFT)
                            qpos = lax.broadcasted_iota(jnp.int32, (SOFT, 2 * pos), 0) + ((2 * blk + c) * pos + r0)
                            kpos = lax.broadcasted_iota(jnp.int32, (SOFT, 2 * pos), 1) + (nk - 2 * pos)
                            last = jnp.minimum(qpos, lv[a, pl.ds(b, 1), 0:2 * pos] - 1)
                            s = sv[rs, nk - 2 * pos:nk] * qscale
                            s = jnp.where(kpos <= last, s, NEG)
                            if blk:
                                s = jnp.concatenate([sv[rs, 0:2 * pos] * qscale, s], axis=1)
                            e = jnp.exp2(s - jnp.max(s, axis=-1, keepdims=True))
                            ov[0, rs, 0:nk] = (e / jnp.sum(e, axis=-1, keepdims=True)).astype(BF)
                    for hd in range(q_heads):
                        head(hd)
                    o = jnp.dot(ov[0, :, 0:nk], vals, preferred_element_type=F32).astype(BF)
                    for hd in range(q_heads):
                        big[sh, row, hd * HEAD:(hd + 1) * HEAD] = o[hd * pos:(hd + 1) * pos]
            loop(0, 2 * seqs, seq)

            @pl.when(jnp.logical_and(giver, l == 0))
            def _():
                loop(0, 2, lambda j: issue_gu(1, j))
            loop(0, 4, lambda s: m_load(s).wait())

            def tau(k):
                return lax.rem(y + lax.div(k, n_half), 2) * n_half + lax.rem(k, n_half)

            def z_store(s, t):
                return local(ov.at[s], z_b.at[l, s, :, tcols(t)], os_.at[0])

            def add_tile(k):
                t = tau(k)
                first = y_goes_first(l, t)

                def total(lhs_ref, rhs_ref):
                    lhs = local(lhs_ref, ab.at[0], ad.at[0])
                    rhs = local(rhs_ref, ab.at[1], ad.at[1])
                    lhs.start()
                    rhs.start()
                    lhs.wait()
                    rhs.wait()

                    def sub(i):
                        rs = pl.ds(pl.multiple_of(i * 128, 128), 128)
                        ab[0, rs, :] = (ab[0, rs, :].astype(F32) + ab[1, rs, :].astype(F32)).astype(BF)
                    loop(0, rows // 128, sub)
                    out = local(ab.at[0], sq.at[l, :, tcols(t)], ad.at[2])
                    out.start()
                    out.wait()

                @pl.when(jnp.logical_not(first))
                def _():
                    xz(l, t, 0).wait_recv()
                    xz(l, t, 1).wait_recv()
                    total(z_b.at[l, 1, :, tcols(t)], xr.at[l, 1, :, tcols(t)])
                    yz(l, t).start()

                @pl.when(first)
                def _():
                    yz_pass(l, t).wait_recv()
                    total(z_b.at[l, 2, :, tcols(t)], ym.at[:, tcols(t)])
                    xz_last(l, t).start()

                @pl.when(jnp.logical_and(giver, jnp.logical_and(l == 0, jnp.logical_and(lax.rem(k, 2) == 1, k >= 3))))
                def _():
                    issue_gu(1, 2 + lax.div(k - 3, 2))

            def out_tile(k):
                slot = lax.rem(k + oslot, 2)
                t = tau(k)
                first = y_goes_first(l, t)
                wait_o(slot)

                def order(si):
                    return si + 2 - lax.div(si, 2) * (2 * si - 1)

                def shard(si):
                    s = order(si)

                    @pl.when(jnp.logical_and(si == 2, k + 1 < n_half))
                    def _():
                        load_o_near(l, k + 1, 1 - slot)

                    @pl.when(jnp.logical_and(si == 2, jnp.logical_and(k + 1 >= n_half, k + 1 < n_out)))
                    def _():
                        arrive_o(l, k + 1 - n_half)
                        load_o(l, r_at, r_ml, k + 1 - n_half, 1 - slot)

                    acc = jnp.dot(big[s], wv[slot], preferred_element_type=F32)
                    ov[s] = acc.astype(BF)

                    @pl.when(jnp.logical_or(si > 0, k > 0))
                    def _():
                        z_store(0, t).wait()

                    @pl.when(jnp.logical_and(jnp.logical_not(first), jnp.logical_and(si >= 1, si < 3)))
                    def _():
                        xz(l, t, si - 1).start()

                    @pl.when(jnp.logical_and(first, si == 2))
                    def _():
                        yz_pass(l, t).start()

                    @pl.when(jnp.logical_and(first, si == 3))
                    def _():
                        yz_first(l, t).start()
                    z_store(s, t).start()
                loop(0, 4, shard)

                @pl.when(jnp.logical_and(k >= 3, lax.rem(k, 2) == 1))
                def _():
                    add_tile(lax.div(k - 3, 2))
            loop(0, n_out, out_tile)
            z_store(0, 0).wait()

            loop(3, n_out, add_tile)

            @pl.when(jnp.logical_and(giver, l == 0))
            def _():
                pass

            @pl.when(l == 0)
            def _():
                loop(0, n_out, lambda t: yz(l, t).wait_recv())
                ln_phase(1)

                @pl.when(giver)
                def _():
                    loop(5, n_gu, lambda j: issue_gu(1, j))
                    issue_qkv(1)
                    loop(0, n_half, lambda t: issue_o(1, t))

            @pl.when(l == 1)
            def _():
                def last_tile(k):
                    t = lax.rem(1 - y + lax.div(k, n_half), 2) * n_half + lax.rem(k, n_half)

                    @pl.when(y_goes_first(l, t))
                    def _():
                        xz(l, t, 0).wait_recv()
                    yz(l, t).wait_recv()
                    parts = (hid.at[:, tcols(t)], z_b.at[l, 0, :, tcols(t)], xr.at[l, 0, :, tcols(t)], yr.at[l, :, tcols(t)])
                    cps = [local(p, ov.at[i], os_.at[i]) for i, p in enumerate(parts)]
                    for cp in cps:
                        cp.start()
                    for cp in cps:
                        cp.wait()

                    def sub(i):
                        rs = pl.ds(pl.multiple_of(i * 64, 64), 64)
                        zs = ov[1, rs, :].astype(F32) + ov[2, rs, :].astype(F32)
                        ov[0, rs, :] = (ov[0, rs, :].astype(F32) + (zs + ov[3, rs, :].astype(F32))).astype(BF)
                    loop(0, rows // 64, sub)
                    out = local(ov.at[0], y_out.at[:, tcols(t)], lo.at[0])
                    out.start()
                    out.wait()
                loop(0, n_out, last_tile)

            def sent_h(b):
                hy(l, b).wait_send()
                hx(l, b).wait_send()
            loop(0, n_hb, sent_h)
            hf(l).wait_send()
            kvx(l).wait_send()

            def sent_z(t):
                xz(l, t, 0).wait_send()
                yz(l, t).wait_send()

                @pl.when(y_goes_first(l, t))
                def _():
                    yz_pass(l, t).wait_send()

                @pl.when(jnp.logical_not(y_goes_first(l, t)))
                def _():
                    xz(l, t, 1).wait_send()
            loop(0, n_out, sent_z)

            @pl.when(giver)
            def _():
                loop(0, n_units, lambda u: wy(l, u).wait_send())

                def sent_o(t):
                    for cp in oy(l, t):
                        cp.wait_send()
                loop(0, n_half, sent_o)

            @pl.when(keeper)
            def _():
                loop(0, n_units, lambda u: wc(l, u).wait_send())

                def sent_o(t):
                    for cp in oc(l, t):
                        cp.wait_send()
                loop(0, n_half, sent_o)
                for cp in acopy(l):
                    cp.wait_send()
        loop(0, 2, layer)

    return kernel


def solution(mesh):
    batch_axes = ('rep', 'data')

    def device_step(x_loc, len_loc, gain_loc, w_in_loc, w_attn_loc, w_mlp_loc):
        seqs, pos, d = x_loc.shape
        rows = seqs * pos
        layers, dh, block_in = w_in_loc.shape
        aw = w_attn_loc.shape[1]
        ff = w_mlp_loc.shape[1]
        n_units = block_in // UNIT
        n_out = d // TILE
        kk = aw + ff
        seq_len = pos * mesh.shape['model']
        lens = jnp.broadcast_to(len_loc[:, None], (seqs, seq_len)).astype(jnp.int32)
        gain = jnp.broadcast_to(gain_loc.astype(F32)[:, None, :], (layers, 8, dh))

        def buf(*shape):
            return jax.ShapeDtypeStruct(shape, BF)

        outs = [buf(rows, d), buf(layers, dh, block_in), buf(layers, aw, dh), buf(layers, ff, dh),
                buf(layers, dh, block_in), buf(layers, aw, dh), buf(layers, ff, dh),
                buf(layers, 4, rows, d), buf(layers, 2, 4, rows, 2 * HEAD), buf(4, rows, aw), buf(4, rows, ff),
                buf(layers, 4, rows, d), buf(layers, 2, rows, d), buf(layers, rows, d), buf(rows, d), buf(layers, rows, d), buf(rows, d)]
        dma = pltpu.SemaphoreType.DMA
        n_hb = rows // 128
        scratch = [pltpu.VMEM((4, rows, kk), BF), pltpu.VMEM((2, kk, TILE), BF), pltpu.VMEM((4, rows, TILE), BF),
                   pltpu.VMEM((2, rows, TILE), BF),
                   pltpu.VMEM((2, 4, 64, d), BF), pltpu.VMEM((2, 64, d), BF), pltpu.VMEM((layers, 8, d), F32),
                   pltpu.VMEM((2, seqs, seq_len), jnp.int32), pltpu.VMEM((2, 2, pos, aw), BF),
                   pltpu.VMEM((2, seq_len, 2 * HEAD), BF), pltpu.VMEM((rows, seq_len), F32),
                   dma((layers, 3)), dma((layers, 3)),
                   dma((layers, n_units)), dma((layers, n_units)), dma((layers, n_units)), dma((layers, n_units)),
                   dma((layers, n_out // 2, 2)), dma((layers, n_out // 2, 2)),
                   dma((layers, n_out // 2, 2)), dma((layers, n_out // 2, 2)),
                   dma((layers, n_hb)), dma((layers, n_hb)), dma((layers, n_hb)), dma((layers, n_hb)),
                   dma((layers,)), dma((layers,)), dma((layers,)), dma((layers,)),
                   dma((layers, n_out, 2)), dma((layers, n_out, 2)), dma((layers, n_out)), dma((layers, n_out)),
                   dma((n_out,)), dma((n_out,)),
                   dma((2,)), dma((2,)), dma((2,)), dma((2, 4)), dma((2,)), dma((2,)), dma((4,)), dma((2, 4)), dma((4,)),
                   dma((2, 6)), dma((4,)), dma((3,))]
        hbm = pl.BlockSpec(memory_space=pl.ANY)
        kernel = make_kernel(rows, seqs, d, dh, block_in, aw, ff, n_units)
        got = pl.pallas_call(
            kernel, out_shape=outs, in_specs=[hbm] * 6, out_specs=[hbm] * len(outs), scratch_shapes=scratch, name='two_layers',
            compiler_params=pltpu.CompilerParams(collective_id=0, has_side_effects=True, vmem_limit_bytes=67_000_000),
        )(x_loc.reshape(rows, d), lens, gain, w_in_loc, w_attn_loc, w_mlp_loc)
        return got[0].reshape(seqs, pos, d)

    return jax.shard_map(device_step, mesh=mesh,
                         in_specs=(P(batch_axes, 'model', None), P(batch_axes), P(None, 'data'), P(None, 'data', 'model'),
                                   P(None, 'model', 'data'), P(None, 'model', 'data')),
                         out_specs=P(batch_axes, 'model', None), check_vma=False)
```

```python
import jax
import jax.numpy as jnp
from jax import lax
from jax.experimental import pallas as pl
from jax.experimental.pallas import tpu as pltpu
from jax.sharding import PartitionSpec as P

EPSILON = 1e-6
HEAD = 128
UNIT = 256
TILE = 512
SOFT = 32
NEG = -1e30
MESH = pl.DeviceIdType.MESH
BF = jnp.bfloat16
F32 = jnp.float32


def make_kernel(rows, seqs, d, dh, block_in, aw, ff, n_units):
    q_heads = aw // HEAD
    ff0 = aw + 2 * HEAD
    n_gu = ff // UNIT
    gate_u = ff0 // UNIT
    up_u = (ff0 + ff) // UNIT
    kv_u = aw // UNIT
    n_q = aw // TILE
    n_out = d // TILE
    n_half = n_out // 2
    pos = rows // seqs
    kk = aw + ff
    lnr = 64
    early0, early1 = 6, 10
    n_own = 2
    n_ln = rows // lnr
    n_hb = n_ln // 2
    hb = 2 * lnr
    qscale = HEAD ** -0.5 * 1.4426950408889634

    def kernel(x, lens, gain, w_in, w_at, w_ml,
               y_out, a_in, a_at, a_ml, r_in, r_at, r_ml, h_all, kvb, q_b, m_b, z_b, xr, sq, ym, yr, hid, o_b,
               big, wv, ov, ab, xin, hst, gv, lv, qv, kvv, sv,
               a_s, a_r, wy_s, wy_r, wc_s, wc_r, oy_s, oy_r, oc_s, oc_r, hy_s, hy_r, hx_s, hx_r, hf_s, hf_r,
               kv_s, kv_r, xz_s, xz_r, yz_s, yz_r, y3_s, y3_r, g_s, g_r, lg, li, lh, lo, hl, ws, os_, ai, ao, ml_s, ol_s, ad):
        rep = lax.axis_index('rep')
        y = lax.axis_index('data')
        m = lax.axis_index('model')
        xx = lax.div(m, 2)
        c = lax.rem(m, 2)
        ypeer = (rep, 1 - y, m)
        xpeer = (rep, y, lax.rem(m + 2, 4))
        cpeer = (rep, y, m + 1 - 2 * c)
        keeper = c == y
        giver = c != y

        def remote(src, dst, ss, rs, dev):
            return pltpu.make_async_remote_copy(src_ref=src, dst_ref=dst, send_sem=ss, recv_sem=rs, device_id=dev,
                                                device_id_type=MESH)

        def local(src, dst, sem):
            return pltpu.make_async_copy(src, dst, sem)

        def loop(lo_, hi_, body):
            def step(i, carry):
                body(i)
                return carry
            lax.fori_loop(lo_, hi_, step, 0)

        def ucols(u):
            return pl.ds(pl.multiple_of(u * UNIT, UNIT), UNIT)

        def tcols(t):
            return pl.ds(pl.multiple_of(t * TILE, TILE), TILE)

        def wy(l, u):
            return remote(w_in.at[l, :, ucols(u)], r_in.at[l, :, ucols(u)], wy_s.at[l, u], wy_r.at[l, u], ypeer)

        def wc(l, u):
            return remote(r_in.at[l, :, ucols(u)], r_in.at[l, :, ucols(u)], wc_s.at[l, u], wc_r.at[l, u], cpeer)

        def oy(l, t):
            return (remote(w_at.at[l, :, tcols(t)], r_at.at[l, :, tcols(t)], oy_s.at[l, t, 0], oy_r.at[l, t, 0], ypeer),
                    remote(w_ml.at[l, :, tcols(t)], r_ml.at[l, :, tcols(t)], oy_s.at[l, t, 1], oy_r.at[l, t, 1], ypeer))

        def oc(l, t):
            return (remote(r_at.at[l, :, tcols(t)], r_at.at[l, :, tcols(t)], oc_s.at[l, t, 0], oc_r.at[l, t, 0], cpeer),
                    remote(r_ml.at[l, :, tcols(t)], r_ml.at[l, :, tcols(t)], oc_s.at[l, t, 1], oc_r.at[l, t, 1], cpeer))

        def acopy(l):
            return (remote(w_in.at[l], a_in.at[l], a_s.at[l, 0], a_r.at[l, 0], cpeer),
                    remote(w_at.at[l], a_at.at[l], a_s.at[l, 1], a_r.at[l, 1], cpeer),
                    remote(w_ml.at[l], a_ml.at[l], a_s.at[l, 2], a_r.at[l, 2], cpeer))

        def hrows(b):
            return pl.ds(pl.multiple_of(b * hb, hb), hb)

        def hy(l, b):
            return remote(h_all.at[l, 0, hrows(b)], h_all.at[l, 1, hrows(b)], hy_s.at[l, b], hy_r.at[l, b], ypeer)

        def hx(l, b):
            return remote(h_all.at[l, 0, hrows(b)], h_all.at[l, 2, hrows(b)], hx_s.at[l, b], hx_r.at[l, b], xpeer)

        def hf(l):
            return remote(h_all.at[l, 1], h_all.at[l, 3], hf_s.at[l], hf_r.at[l], xpeer)

        def kvx(l, a):
            return remote(kvb.at[l, 0, a], kvb.at[l, 1, a], kv_s.at[l, a], kv_r.at[l, a], cpeer)

        def xz(l, t, i):
            return remote(z_b.at[l, 2 + i, :, tcols(t)], xr.at[l, i, :, tcols(t)], xz_s.at[l, t, i], xz_r.at[l, t, i], xpeer)

        def yz(l, t):
            return remote(sq.at[l, :, tcols(t)], yr.at[l, :, tcols(t)], yz_s.at[l, t], yz_r.at[l, t], ypeer)

        def yz_first(l, t):
            return remote(z_b.at[l, 1, :, tcols(t)], yr.at[l, :, tcols(t)], yz_s.at[l, t], yz_r.at[l, t], ypeer)

        def yz_pass(l, t):
            return remote(z_b.at[l, 3, :, tcols(t)], ym.at[:, tcols(t)], y3_s.at[t], y3_r.at[t], ypeer)

        def xz_last(l, t):
            return remote(sq.at[l, :, tcols(t)], xr.at[l, 0, :, tcols(t)], xz_s.at[l, t, 0], xz_r.at[l, t, 0], xpeer)

        def y_goes_first(l, t):
            return jnp.logical_and(l == 1, lax.rem(t, n_half) == n_half - 1)

        def issue_gu(l, j):
            wy(l, gate_u + j).start()
            wy(l, up_u + j).start()

        def issue_kv(l):
            wy(l, kv_u).start()

        def issue_q(l, u_lo):
            loop(u_lo, kv_u, lambda u: wy(l, u).start())

        def issue_o(l, t):
            for cp in oy(l, t):
                cp.start()

        def arrive(l, u):
            @pl.when(keeper)
            def _():
                wy(l, u).wait_recv()
                wc(l, u).start()

            @pl.when(giver)
            def _():
                wc(l, u).wait_recv()

        def arrive_o(l, t):
            @pl.when(keeper)
            def _():
                for cp, fw in zip(oy(l, t), oc(l, t)):
                    cp.wait_recv()
                    fw.start()

            @pl.when(giver)
            def _():
                for fw in oc(l, t):
                    fw.wait_recv()

        def near_in(l, u, slot, half):
            return wv.at[slot, pl.ds(pl.multiple_of(y * dh, dh), dh), half * UNIT:(half + 1) * UNIT]

        def load_unit(l, u, slot, half):
            near = wv.at[slot, pl.ds(pl.multiple_of(y * dh, dh), dh), half * UNIT:(half + 1) * UNIT]
            far = wv.at[slot, pl.ds(pl.multiple_of((1 - y) * dh, dh), dh), half * UNIT:(half + 1) * UNIT]

            @pl.when(keeper)
            def _():
                local(w_in.at[l, :, ucols(u)], near, ws.at[slot, half]).start()

            @pl.when(giver)
            def _():
                local(a_in.at[l, :, ucols(u)], near, ws.at[slot, half]).start()

            local(r_in.at[l, :, ucols(u)], far, ws.at[slot, 2 + half]).start()

        def wait_unit(slot, half):
            near = wv.at[slot, pl.ds(pl.multiple_of(y * dh, dh), dh), half * UNIT:(half + 1) * UNIT]
            far = wv.at[slot, pl.ds(pl.multiple_of((1 - y) * dh, dh), dh), half * UNIT:(half + 1) * UNIT]
            local(r_in.at[0, :, ucols(0)], near, ws.at[slot, half]).wait()
            local(r_in.at[0, :, ucols(0)], far, ws.at[slot, 2 + half]).wait()

        def load_o(l, src_at, src_ml, t, slot):
            local(src_at.at[l, :, tcols(t)], wv.at[slot, 0:aw], ws.at[slot, 0]).start()
            local(src_ml.at[l, :, tcols(t)], wv.at[slot, aw:kk], ws.at[slot, 1]).start()

        def load_o_near(l, t, slot):
            @pl.when(keeper)
            def _():
                load_o(l, w_at, w_ml, t, slot)

            @pl.when(giver)
            def _():
                load_o(l, a_at, a_ml, t, slot)

        def wait_o(slot):
            local(r_at.at[0, :, tcols(0)], wv.at[slot, 0:aw], ws.at[slot, 0]).wait()
            local(r_ml.at[0, :, tcols(0)], wv.at[slot, aw:kk], ws.at[slot, 1]).wait()

        def lrows(r):
            return pl.ds(pl.multiple_of(r * lnr, lnr), lnr)

        def ln_phase(kind):
            ln = kind
            srcs = [x, z_b.at[0, 0], xr.at[0, 0], yr.at[0]] if kind else [x]

            def loads(r, slot):
                return [local(s.at[lrows(r)], xin.at[slot, i], li.at[slot, i]) for i, s in enumerate(srcs)]

            def store_h(r, slot):
                return local(big.at[0, lrows(r), 0:d], h_all.at[ln, 0, lrows(r)], lh.at[slot])

            def store_o(r, slot):
                return local(hst.at[slot], hid.at[lrows(r)], lo.at[slot])

            def send(b):
                hy(ln, b).start()
                hx(ln, b).start()

            for cp in loads(0, 0):
                cp.start()

            def block(r):
                slot = lax.rem(r, 2)

                @pl.when(r + 1 < n_ln)
                def _():
                    for cp in loads(r + 1, 1 - slot):
                        cp.start()
                for cp in loads(r, slot):
                    cp.wait()
                if kind > 0:
                    @pl.when(r >= 2)
                    def _():
                        store_o(r - 2, slot).wait()

                def sub(i):
                    rs = pl.ds(pl.multiple_of(i * 32, 32), 32)
                    v = xin[slot, 0, rs, :].astype(F32)
                    if kind > 0:
                        zs = xin[slot, 1, rs, :].astype(F32) + xin[slot, 2, rs, :].astype(F32)
                        v = (v + (zs + xin[slot, 3, rs, :].astype(F32))).astype(BF)
                        hst[slot, rs, :] = v
                        v = v.astype(F32)
                    if True:
                        mean = jnp.sum(v, axis=-1, keepdims=True) * (1.0 / d)
                        cen = v - mean
                        var = jnp.sum(cen * cen, axis=-1, keepdims=True) * (1.0 / d)
                        out = cen * lax.rsqrt(var + EPSILON) * gv[ln, 0:1, :]
                        big[0, pl.ds(pl.multiple_of(r * lnr + i * 32, 32), 32), 0:d] = out.astype(BF)
                loop(0, lnr // 32, sub)
                if kind > 0:
                    store_o(r, slot).start()
                if True:
                    store_h(r, slot).start()

                    @pl.when(r >= 1)
                    def _():
                        store_h(r - 1, 1 - slot).wait()

                    @pl.when(jnp.logical_and(r >= 2, lax.rem(r, 2) == 0))
                    def _():
                        send(lax.div(r, 2) - 1)
            loop(0, n_ln, block)
            if kind > 0:
                store_o(n_ln - 2, 0).wait()
                store_o(n_ln - 1, 1).wait()
            store_h(n_ln - 1, 1).wait()
            send(n_hb - 1)

        barrier = pltpu.get_barrier_semaphore()
        for dev in (ypeer, xpeer, cpeer):
            pl.semaphore_signal(barrier, inc=1, device_id=dev, device_id_type=MESH)
        pl.semaphore_wait(barrier, 3)

        def gain_y():
            half = gv.at[:, :, pl.ds(pl.multiple_of(y * dh, dh), dh)]
            return remote(gain, half, g_s.at[0], g_r.at[0], ypeer)

        def lens_y():
            return remote(lens, lv.at[1], g_s.at[1], g_r.at[1], ypeer)

        def gain_l():
            return local(gain, gv.at[:, :, pl.ds(pl.multiple_of(y * dh, dh), dh)], lg.at[0])

        def lens_l():
            return local(lens, lv.at[0], lg.at[1])

        gain_y().start()
        lens_y().start()
        gain_l().start()
        lens_l().start()

        @pl.when(keeper)
        def _():
            for l in range(2):
                for cp in acopy(l):
                    cp.start()

        @pl.when(giver)
        def _():
            issue_kv(0)
            wy(0, 0).start()
        gain_l().wait()
        lens_l().wait()
        gain_y().wait()
        lens_y().wait()
        ln_phase(0)

        @pl.when(giver)
        def _():
            issue_q(0, 1)
            loop(0, n_gu, lambda j: issue_gu(0, j))
            loop(0, n_half, lambda t: issue_o(0, t))

        def layer(l):
            @pl.when(giver)
            def _():
                for cp in acopy(l):
                    cp.wait_recv()

            def h_load(s):
                return local(h_all.at[l, s], big.at[s, :, 0:d], hl.at[s])

            def m_store(s, j, buf):
                return local(ov.at[buf, :, 0:UNIT], m_b.at[s, :, ucols(j)], os_.at[0])

            def q_store(s, t, buf):
                return local(ov.at[buf], q_b.at[s, :, tcols(t)], os_.at[0])

            def kv_store(s, buf):
                return local(ov.at[buf, :, 0:UNIT], kvb.at[l, 0, lax.rem(s, 2), lax.div(s, 2)], os_.at[0])

            def wait_half():
                m_store(0, 0, 0).wait()

            def wait_full():
                q_store(0, 0, 0).wait()

            def arrive_gu(j):
                arrive(l, gate_u + j)
                arrive(l, up_u + j)

            def load_gu(j, slot):
                load_unit(l, gate_u + j, slot, 0)
                load_unit(l, up_u + j, slot, 1)

            def arrive_q(t):
                arrive(l, 2 * t)
                arrive(l, 2 * t + 1)

            def load_q(t, slot):
                load_unit(l, 2 * t, slot, 0)
                load_unit(l, 2 * t + 1, slot, 1)

            def load_kv(slot):
                load_unit(l, kv_u, slot, 0)

            def wait_tile(slot):
                wait_unit(slot, 0)
                wait_unit(slot, 1)

            def gu_step(s, j, slot, before, buf):
                acc = jnp.dot(big[s, :, 0:d], wv[slot, 0:d, :], preferred_element_type=F32)
                g = acc[:, :UNIT].astype(BF).astype(F32)
                u = acc[:, UNIT:].astype(BF).astype(F32)
                ov[buf, :, 0:UNIT] = (g * jax.nn.sigmoid(g) * u).astype(BF)
                before()
                m_store(s, j, buf).start()

            def q_step(s, t, slot, before, buf):
                ov[buf] = jnp.dot(big[s, :, 0:d], wv[slot, 0:d, :], preferred_element_type=F32).astype(BF)
                before()
                q_store(s, t, buf).start()

            def kv_step(s, slot, before, buf):
                ov[buf, :, 0:UNIT] = jnp.dot(big[s, :, 0:d], wv[slot, 0:d, 0:UNIT], preferred_element_type=F32).astype(BF)
                before()
                kv_store(s, buf).start()

            def nothing():
                pass

            def either(cond, yes, no):
                def go():
                    pl.when(cond)(yes)
                    pl.when(jnp.logical_not(cond))(no)
                return go

            def unless(cond, no):
                return lambda: pl.when(jnp.logical_not(cond))(no)

            @pl.when(l == 0)
            def _():
                arrive(l, kv_u)
                load_kv(0)

            @pl.when(l == 1)
            def _():
                arrive(l, kv_u)
                load_kv(0)
                arrive_q(0)
                load_q(0, 1)
                wait_unit(0, 0)
                kv_step(0, 0, nothing, 0)

                def own_q(t):
                    slot = lax.rem(1 + t, 2)

                    @pl.when(t + 1 < n_q)
                    def _():
                        arrive_q(t + 1)
                        load_q(t + 1, 1 - slot)

                    @pl.when(t + 1 == n_q)
                    def _():
                        arrive_gu(0)
                        load_gu(0, 1 - slot)
                    wait_tile(slot)
                    q_step(0, t, slot, either(t == 0, wait_half, wait_full), slot)
                loop(0, n_q, own_q)

                def own_gu(j):
                    slot = lax.rem(1 + j, 2)

                    @pl.when(j + 1 < n_own)
                    def _():
                        arrive_gu(j + 1)
                        load_gu(j + 1, 1 - slot)
                    wait_tile(slot)
                    gu_step(0, j, slot, either(j == 0, wait_full, wait_half), slot)
                loop(0, n_own, own_gu)
                wait_half()
                load_kv(0)

            loop(0, n_hb, lambda b: hy(l, b).wait_recv())
            hf(l).start()
            h_load(1).start()
            loop(0, n_hb, lambda b: hx(l, b).wait_recv())
            h_load(2).start()
            h_load(1).wait()
            h_load(2).wait()

            wait_unit(0, 0)

            def kv_a(s):
                @pl.when(s == 1)
                def _():
                    pl.when(l == 0)(lambda: arrive_q(0))
                    load_q(0, 1)
                kv_step(s, 0, unless(s == l, wait_half), s)
            loop(l, 3, kv_a)

            def q_a(t):
                slot = lax.rem(1 + t, 2)
                wait_tile(slot)

                def shard(s):
                    @pl.when(jnp.logical_and(s == 1, t + 1 < n_q))
                    def _():
                        pl.when(l == 0)(lambda: arrive_q(t + 1))
                        load_q(t + 1, 1 - slot)
                    q_step(s, t, slot, either(jnp.logical_and(t == 0, s == l), wait_half, wait_full), s)
                loop(l, 3, shard)

                @pl.when(t == 0)
                def _():
                    kvx(l, 0).start()
            loop(0, n_q, q_a)
            wait_full()

            def attend(a, middle):
                kvx(l, a).wait_recv()

                def at_loads(b, slot):
                    rs = pl.ds(pl.multiple_of(b * pos, pos), pos)

                    def at(quarter):
                        return kvv.at[slot, pl.ds(pl.multiple_of(quarter * pos, pos), pos)]
                    return (local(q_b.at[a, rs], qv.at[slot, xx], ai.at[slot, 0]),
                            local(q_b.at[2 + a, rs], qv.at[slot, 1 - xx], ai.at[slot, 1]),
                            local(kvb.at[l, 0, a, 0, rs], at(2 * xx + c), ai.at[slot, 2]),
                            local(kvb.at[l, 0, a, 1, rs], at(2 * (1 - xx) + c), ai.at[slot, 3]),
                            local(kvb.at[l, 1, a, 0, rs], at(2 * xx + 1 - c), ai.at[slot, 4]),
                            local(kvb.at[l, 1, a, 1, rs], at(2 * (1 - xx) + 1 - c), ai.at[slot, 5]))

                def o_stores(b, slot):
                    rs = pl.ds(pl.multiple_of(b * pos, pos), pos)
                    out = []
                    for blk in range(2):
                        sh = a + 2 * (blk + xx - 2 * blk * xx)
                        for i in range(n_q):
                            n = blk * n_q + i
                            out.append(local(ab.at[slot, n * pos:(n + 1) * pos], o_b.at[sh, rs, i * TILE:(i + 1) * TILE], ao.at[slot, n]))
                    return out

                for cp in at_loads(0, 0):
                    cp.start()

                def seq(b):
                    slot = lax.rem(b, 2)

                    @pl.when(b + 1 < seqs)
                    def _():
                        for cp in at_loads(b + 1, 1 - slot):
                            cp.start()
                    pl.when(b == seqs // 2)(middle)
                    for cp in at_loads(b, slot):
                        cp.wait()

                    @pl.when(b >= 2)
                    def _():
                        for cp in o_stores(b - 2, slot):
                            cp.wait()
                    for blk in range(2):
                        nk = 2 * pos * (blk + 1)
                        keys = kvv[slot, 0:nk, 0:HEAD]
                        vals = kvv[slot, 0:nk, HEAD:2 * HEAD]
                        q_all = jnp.concatenate([qv[slot, blk, :, hd * HEAD:(hd + 1) * HEAD] for hd in range(q_heads)], axis=0)
                        sv[:, 0:nk] = lax.dot_general(q_all, keys, (((1,), (1,)), ((), ())), preferred_element_type=F32)
                        for r0 in range(0, rows, SOFT):
                            rs = slice(r0, r0 + SOFT)
                            qpos = lax.broadcasted_iota(jnp.int32, (SOFT, 2 * pos), 0) + ((2 * blk + c) * pos + r0 % pos)
                            kpos = lax.broadcasted_iota(jnp.int32, (SOFT, 2 * pos), 1) + (nk - 2 * pos)
                            last = jnp.minimum(qpos, lv[a, pl.ds(b, 1), 0:2 * pos] - 1)
                            s = sv[rs, nk - 2 * pos:nk] * qscale
                            s = jnp.where(kpos <= last, s, NEG)
                            if blk:
                                s = jnp.concatenate([sv[rs, 0:2 * pos] * qscale, s], axis=1)
                            e = jnp.exp2(s - jnp.max(s, axis=-1, keepdims=True))
                            ov[0, rs, 0:nk] = (e / jnp.sum(e, axis=-1, keepdims=True)).astype(BF)
                        o = jnp.dot(ov[0, :, 0:nk], vals, preferred_element_type=F32).astype(BF)
                        per = TILE // HEAD
                        for hd in range(q_heads):
                            n = blk * n_q + hd // per
                            ab[slot, n * pos:(n + 1) * pos, (hd % per) * HEAD:(hd % per + 1) * HEAD] = o[hd * pos:(hd + 1) * pos]
                    for cp in o_stores(b, slot):
                        cp.start()
                loop(0, seqs, seq)
                for b in (seqs - 2, seqs - 1):
                    for cp in o_stores(b, b % 2):
                        cp.wait()

            def first_gu():
                pl.when(l == 0)(lambda: arrive_gu(0))
                load_gu(0, 1)
            attend(0, first_gu)

            early = early0 + (early1 - early0) * l

            def gu_a(j):
                slot = lax.rem(1 + j, 2)
                s_lo = l * lax.max(1 - lax.div(j, n_own), 0)
                wait_tile(slot)

                def shard(s):
                    @pl.when(jnp.logical_and(s == 1, j + 1 < early))
                    def _():
                        pl.when(jnp.logical_or(l == 0, j + 1 >= n_own))(lambda: arrive_gu(j + 1))
                        load_gu(j + 1, 1 - slot)

                    @pl.when(jnp.logical_and(s == 1, j + 1 == early))
                    def _():
                        load_kv(1)
                    gu_step(s, j, slot, unless(jnp.logical_and(j == 0, s == s_lo), wait_half), s)
                loop(s_lo, 3, shard)
            loop(0, early, gu_a)

            hf(l).wait_recv()
            h_load(3).start()
            load_q(0, 0)
            wait_unit(1, 0)
            h_load(3).wait()
            kv_step(3, 1, wait_half, 3)

            def q_b3(t):
                slot = lax.rem(t, 2)

                @pl.when(t + 1 < n_q)
                def _():
                    load_q(t + 1, 1 - slot)

                @pl.when(t + 1 == n_q)
                def _():
                    load_gu(0, 1 - slot)
                wait_tile(slot)
                q_step(3, t, slot, either(t == 0, wait_half, wait_full), 2 + slot)

                @pl.when(t == 0)
                def _():
                    kvx(l, 1).start()
            loop(0, n_q, q_b3)

            def gu_b(j):
                slot = lax.rem(j, 2)

                @pl.when(j + 1 < early)
                def _():
                    load_gu(j + 1, 1 - slot)

                @pl.when(j + 1 == early)
                def _():
                    arrive_gu(early)
                    load_gu(early, 1 - slot)
                wait_tile(slot)
                gu_step(3, j, slot, either(j == 0, wait_full, wait_half), 2 + slot)
            loop(0, early, gu_b)
            wait_half()
            attend(1, nothing)

            def gu_c(j):
                slot = lax.rem(j, 2)
                wait_tile(slot)

                def shard(s):
                    @pl.when(jnp.logical_and(s == 2, j + 1 < n_gu))
                    def _():
                        arrive_gu(j + 1)
                        load_gu(j + 1, 1 - slot)

                    @pl.when(jnp.logical_and(s == 2, j + 1 == n_gu))
                    def _():
                        load_o_near(l, 0, 1 - slot)
                    gu_step(s, j, slot, unless(jnp.logical_and(j == early, s == 0), wait_half), s)
                loop(0, 4, shard)
            loop(early, n_gu, gu_c)
            wait_half()
            oslot = n_gu % 2

            def om_load(s):
                return (local(o_b.at[s], big.at[s, :, 0:aw], ol_s.at[s]), local(m_b.at[s], big.at[s, :, aw:kk], ml_s.at[s]))
            for s in (2, 3, 1, 0):
                for cp in om_load(s):
                    cp.start()

            @pl.when(jnp.logical_and(giver, l == 0))
            def _():
                issue_kv(1)
                issue_q(1, 0)

            def tau(k):
                return lax.rem(y + lax.div(k, n_half), 2) * n_half + lax.rem(k, n_half)

            def z_store(s, t):
                return local(ov.at[s], z_b.at[l, s, :, tcols(t)], os_.at[0])

            def add_tile(k):
                t = tau(k)
                first = y_goes_first(l, t)

                def total(lhs_ref, rhs_ref):
                    lhs = local(lhs_ref, ab.at[0], ad.at[0])
                    rhs = local(rhs_ref, ab.at[1], ad.at[1])
                    lhs.start()
                    rhs.start()
                    lhs.wait()
                    rhs.wait()

                    def sub(i):
                        rs = pl.ds(pl.multiple_of(i * 128, 128), 128)
                        ab[0, rs, :] = (ab[0, rs, :].astype(F32) + ab[1, rs, :].astype(F32)).astype(BF)
                    loop(0, rows // 128, sub)
                    out = local(ab.at[0], sq.at[l, :, tcols(t)], ad.at[2])
                    out.start()
                    out.wait()

                @pl.when(jnp.logical_not(first))
                def _():
                    xz(l, t, 0).wait_recv()
                    xz(l, t, 1).wait_recv()
                    total(z_b.at[l, 1, :, tcols(t)], xr.at[l, 1, :, tcols(t)])
                    yz(l, t).start()

                @pl.when(first)
                def _():
                    yz_pass(l, t).wait_recv()
                    total(z_b.at[l, 2, :, tcols(t)], ym.at[:, tcols(t)])
                    xz_last(l, t).start()

                @pl.when(jnp.logical_and(giver, jnp.logical_and(l == 0, jnp.logical_and(lax.rem(k, 2) == 1, k >= 3))))
                def _():
                    issue_gu(1, lax.div(k - 3, 2))

            def out_tile(k):
                slot = lax.rem(k + oslot, 2)
                t = tau(k)
                first = y_goes_first(l, t)
                wait_o(slot)

                def order(si):
                    return si + 2 - lax.div(si, 2) * (2 * si - 1)

                def shard(si):
                    s = order(si)

                    @pl.when(jnp.logical_and(si == 2, k + 1 < n_half))
                    def _():
                        load_o_near(l, k + 1, 1 - slot)

                    @pl.when(jnp.logical_and(si == 2, jnp.logical_and(k + 1 >= n_half, k + 1 < n_out)))
                    def _():
                        arrive_o(l, k + 1 - n_half)
                        load_o(l, r_at, r_ml, k + 1 - n_half, 1 - slot)

                    @pl.when(k == 0)
                    def _():
                        for cp in om_load(s):
                            cp.wait()
                    acc = jnp.dot(big[s], wv[slot], preferred_element_type=F32)
                    ov[s] = acc.astype(BF)

                    @pl.when(jnp.logical_or(si > 0, k > 0))
                    def _():
                        z_store(0, t).wait()

                    @pl.when(jnp.logical_and(jnp.logical_not(first), jnp.logical_and(si >= 1, si < 3)))
                    def _():
                        xz(l, t, si - 1).start()

                    @pl.when(jnp.logical_and(first, si == 2))
                    def _():
                        yz_pass(l, t).start()

                    @pl.when(jnp.logical_and(first, si == 3))
                    def _():
                        yz_first(l, t).start()
                    z_store(s, t).start()
                loop(0, 4, shard)

                @pl.when(jnp.logical_and(k >= 3, lax.rem(k, 2) == 1))
                def _():
                    add_tile(lax.div(k - 3, 2))
            loop(0, n_out, out_tile)
            z_store(0, 0).wait()

            loop(3, n_out, add_tile)

            @pl.when(jnp.logical_and(giver, l == 0))
            def _():
                pass

            @pl.when(l == 0)
            def _():
                loop(0, n_out, lambda t: yz(l, t).wait_recv())
                ln_phase(1)

                @pl.when(giver)
                def _():
                    loop(3, n_gu, lambda j: issue_gu(1, j))
                    loop(0, n_half, lambda t: issue_o(1, t))

            @pl.when(l == 1)
            def _():
                def last_tile(k):
                    t = lax.rem(1 - y + lax.div(k, n_half), 2) * n_half + lax.rem(k, n_half)

                    @pl.when(y_goes_first(l, t))
                    def _():
                        xz(l, t, 0).wait_recv()
                    yz(l, t).wait_recv()
                    parts = (hid.at[:, tcols(t)], z_b.at[l, 0, :, tcols(t)], xr.at[l, 0, :, tcols(t)], yr.at[l, :, tcols(t)])
                    cps = [local(p, ov.at[i], os_.at[i]) for i, p in enumerate(parts)]
                    for cp in cps:
                        cp.start()
                    for cp in cps:
                        cp.wait()

                    def sub(i):
                        rs = pl.ds(pl.multiple_of(i * 64, 64), 64)
                        zs = ov[1, rs, :].astype(F32) + ov[2, rs, :].astype(F32)
                        ov[0, rs, :] = (ov[0, rs, :].astype(F32) + (zs + ov[3, rs, :].astype(F32))).astype(BF)
                    loop(0, rows // 64, sub)
                    out = local(ov.at[0], y_out.at[:, tcols(t)], lo.at[0])
                    out.start()
                    out.wait()
                loop(0, n_out, last_tile)

            def sent_h(b):
                hy(l, b).wait_send()
                hx(l, b).wait_send()
            loop(0, n_hb, sent_h)
            hf(l).wait_send()
            for a in range(2):
                kvx(l, a).wait_send()

            def sent_z(t):
                xz(l, t, 0).wait_send()
                yz(l, t).wait_send()

                @pl.when(y_goes_first(l, t))
                def _():
                    yz_pass(l, t).wait_send()

                @pl.when(jnp.logical_not(y_goes_first(l, t)))
                def _():
                    xz(l, t, 1).wait_send()
            loop(0, n_out, sent_z)

            @pl.when(giver)
            def _():
                loop(0, n_units, lambda u: wy(l, u).wait_send())

                def sent_o(t):
                    for cp in oy(l, t):
                        cp.wait_send()
                loop(0, n_half, sent_o)

            @pl.when(keeper)
            def _():
                loop(0, n_units, lambda u: wc(l, u).wait_send())

                def sent_o(t):
                    for cp in oc(l, t):
                        cp.wait_send()
                loop(0, n_half, sent_o)
                for cp in acopy(l):
                    cp.wait_send()
        loop(0, 2, layer)

    return kernel


def solution(mesh):
    batch_axes = ('rep', 'data')

    def device_step(x_loc, len_loc, gain_loc, w_in_loc, w_attn_loc, w_mlp_loc):
        seqs, pos, d = x_loc.shape
        rows = seqs * pos
        layers, dh, block_in = w_in_loc.shape
        aw = w_attn_loc.shape[1]
        ff = w_mlp_loc.shape[1]
        n_units = block_in // UNIT
        n_out = d // TILE
        kk = aw + ff
        seq_len = pos * mesh.shape['model']
        lens = jnp.broadcast_to(len_loc[:, None], (seqs, seq_len)).astype(jnp.int32)
        gain = jnp.broadcast_to(gain_loc.astype(F32)[:, None, :], (layers, 8, dh))

        def buf(*shape):
            return jax.ShapeDtypeStruct(shape, BF)

        outs = [buf(rows, d), buf(layers, dh, block_in), buf(layers, aw, dh), buf(layers, ff, dh),
                buf(layers, dh, block_in), buf(layers, aw, dh), buf(layers, ff, dh),
                buf(layers, 4, rows, d), buf(layers, 2, 2, 2, rows, 2 * HEAD), buf(4, rows, aw), buf(4, rows, ff),
                buf(layers, 4, rows, d), buf(layers, 2, rows, d), buf(layers, rows, d), buf(rows, d), buf(layers, rows, d), buf(rows, d),
                buf(4, rows, aw)]
        dma = pltpu.SemaphoreType.DMA
        n_hb = rows // 128
        scratch = [pltpu.VMEM((4, rows, kk), BF), pltpu.VMEM((2, kk, TILE), BF), pltpu.VMEM((4, rows, TILE), BF),
                   pltpu.VMEM((2, rows, TILE), BF),
                   pltpu.VMEM((2, 4, 64, d), BF), pltpu.VMEM((2, 64, d), BF), pltpu.VMEM((layers, 8, d), F32),
                   pltpu.VMEM((2, seqs, seq_len), jnp.int32), pltpu.VMEM((2, 2, pos, aw), BF),
                   pltpu.VMEM((2, seq_len, 2 * HEAD), BF), pltpu.VMEM((rows, seq_len), F32),
                   dma((layers, 3)), dma((layers, 3)),
                   dma((layers, n_units)), dma((layers, n_units)), dma((layers, n_units)), dma((layers, n_units)),
                   dma((layers, n_out // 2, 2)), dma((layers, n_out // 2, 2)),
                   dma((layers, n_out // 2, 2)), dma((layers, n_out // 2, 2)),
                   dma((layers, n_hb)), dma((layers, n_hb)), dma((layers, n_hb)), dma((layers, n_hb)),
                   dma((layers,)), dma((layers,)), dma((layers, 2)), dma((layers, 2)),
                   dma((layers, n_out, 2)), dma((layers, n_out, 2)), dma((layers, n_out)), dma((layers, n_out)),
                   dma((n_out,)), dma((n_out,)),
                   dma((2,)), dma((2,)), dma((2,)), dma((2, 4)), dma((2,)), dma((2,)), dma((4,)), dma((2, 4)), dma((4,)),
                   dma((2, 6)), dma((2, 2 * (aw // TILE))), dma((4,)), dma((4,)), dma((3,))]
        hbm = pl.BlockSpec(memory_space=pl.ANY)
        kernel = make_kernel(rows, seqs, d, dh, block_in, aw, ff, n_units)
        got = pl.pallas_call(
            kernel, out_shape=outs, in_specs=[hbm] * 6, out_specs=[hbm] * len(outs), scratch_shapes=scratch, name='two_layers',
            compiler_params=pltpu.CompilerParams(collective_id=0, has_side_effects=True, vmem_limit_bytes=67_000_000),
        )(x_loc.reshape(rows, d), lens, gain, w_in_loc, w_attn_loc, w_mlp_loc)
        return got[0].reshape(seqs, pos, d)

    return jax.shard_map(device_step, mesh=mesh,
                         in_specs=(P(batch_axes, 'model', None), P(batch_axes), P(None, 'data'), P(None, 'data', 'model'),
                                   P(None, 'model', 'data'), P(None, 'model', 'data')),
                         out_specs=P(batch_axes, 'model', None), check_vma=False)
```

```python
import jax
import jax.numpy as jnp
from jax import lax
from jax.experimental import pallas as pl
from jax.experimental.pallas import tpu as pltpu
from jax.sharding import PartitionSpec as P

EPSILON = 1e-6
HEAD = 128
UNIT = 256
TILE = 512
SOFT = 32
NEG = -1e30
MESH = pl.DeviceIdType.MESH
BF = jnp.bfloat16
F32 = jnp.float32


def make_kernel(rows, seqs, d, dh, block_in, aw, ff, n_units):
    q_heads = aw // HEAD
    ff0 = aw + 2 * HEAD
    n_gu = ff // UNIT
    gate_u = ff0 // UNIT
    up_u = (ff0 + ff) // UNIT
    kv_u = aw // UNIT
    n_q = aw // TILE
    n_out = d // TILE
    n_half = n_out // 2
    pos = rows // seqs
    kk = aw + ff
    lnr = 64
    early0, late0, early1, late1 = 2, 6, 6, 10
    n_own = 2
    n_ln = rows // lnr
    n_hb = n_ln // 2
    hb = 2 * lnr
    hr = rows // 2
    qscale = HEAD ** -0.5 * 1.4426950408889634

    def kernel(x, lens, gain, w_in, w_at, w_ml,
               y_out, a_in, a_at, a_ml, r_in, r_at, r_ml, h_all, kvb, q_b, m_b, z_b, xr, sq, yr, hid, o_b,
               big, wv, ov, ab, xin, hst, gv, lv, qv, kvv, sv,
               a_s, a_r, wy_s, wy_r, wc_s, wc_r, oy_s, oy_r, oc_s, oc_r, hy_s, hy_r, hx_s, hx_r, hf_s, hf_r,
               kv_s, kv_r, xz_s, xz_r, yz_s, yz_r, g_s, g_r, lg, li, lh, lo, hl, ws, os_, ai, ao, ml_s, ol_s, ad):
        rep = lax.axis_index('rep')
        y = lax.axis_index('data')
        m = lax.axis_index('model')
        xx = lax.div(m, 2)
        c = lax.rem(m, 2)
        ypeer = (rep, 1 - y, m)
        xpeer = (rep, y, lax.rem(m + 2, 4))
        cpeer = (rep, y, m + 1 - 2 * c)
        keeper = c == y
        giver = c != y

        def remote(src, dst, ss, rs, dev):
            return pltpu.make_async_remote_copy(src_ref=src, dst_ref=dst, send_sem=ss, recv_sem=rs, device_id=dev,
                                                device_id_type=MESH)

        def local(src, dst, sem):
            return pltpu.make_async_copy(src, dst, sem)

        def loop(lo_, hi_, body):
            def step(i, carry):
                body(i)
                return carry
            lax.fori_loop(lo_, hi_, step, 0)

        def ucols(u):
            return pl.ds(pl.multiple_of(u * UNIT, UNIT), UNIT)

        def tcols(t):
            return pl.ds(pl.multiple_of(t * TILE, TILE), TILE)

        def wy(l, u):
            return remote(w_in.at[l, :, ucols(u)], r_in.at[l, :, ucols(u)], wy_s.at[l, u], wy_r.at[l, u], ypeer)

        def wc(l, u):
            return remote(r_in.at[l, :, ucols(u)], r_in.at[l, :, ucols(u)], wc_s.at[l, u], wc_r.at[l, u], cpeer)

        def oy(l, t):
            return (remote(w_at.at[l, :, tcols(t)], r_at.at[l, :, tcols(t)], oy_s.at[l, t, 0], oy_r.at[l, t, 0], ypeer),
                    remote(w_ml.at[l, :, tcols(t)], r_ml.at[l, :, tcols(t)], oy_s.at[l, t, 1], oy_r.at[l, t, 1], ypeer))

        def oc(l, t):
            return (remote(r_at.at[l, :, tcols(t)], r_at.at[l, :, tcols(t)], oc_s.at[l, t, 0], oc_r.at[l, t, 0], cpeer),
                    remote(r_ml.at[l, :, tcols(t)], r_ml.at[l, :, tcols(t)], oc_s.at[l, t, 1], oc_r.at[l, t, 1], cpeer))

        def acopy(l):
            return (remote(w_in.at[l], a_in.at[l], a_s.at[l, 0], a_r.at[l, 0], cpeer),
                    remote(w_at.at[l], a_at.at[l], a_s.at[l, 1], a_r.at[l, 1], cpeer),
                    remote(w_ml.at[l], a_ml.at[l], a_s.at[l, 2], a_r.at[l, 2], cpeer))

        def hrows(b):
            return pl.ds(pl.multiple_of(b * hb, hb), hb)

        def hy(l, b):
            return remote(h_all.at[l, 0, hrows(b)], h_all.at[l, 1, hrows(b)], hy_s.at[l, b], hy_r.at[l, b], ypeer)

        def hx(l, b):
            return remote(h_all.at[l, 0, hrows(b)], h_all.at[l, 2, hrows(b)], hx_s.at[l, b], hx_r.at[l, b], xpeer)

        def hhalf(g):
            return pl.ds(pl.multiple_of(g * hr, hr), hr)

        def hf(l, g):
            return remote(h_all.at[l, 1, hhalf(g)], h_all.at[l, 3, hhalf(g)], hf_s.at[l, g], hf_r.at[l, g], xpeer)

        def kvx(l, a):
            return remote(kvb.at[l, 0, a], kvb.at[l, 1, a], kv_s.at[l, a], kv_r.at[l, a], cpeer)

        def xz(l, w, i):
            return remote(z_b.at[l, 2 + i, :, ucols(w)], xr.at[l, i, :, ucols(w)], xz_s.at[l, w, i], xz_r.at[l, w, i], xpeer)

        def yz(l, w):
            return remote(sq.at[l, :, ucols(w)], yr.at[l, :, ucols(w)], yz_s.at[l, w], yz_r.at[l, w], ypeer)

        def issue_gu(l, j):
            wy(l, gate_u + j).start()
            wy(l, up_u + j).start()

        def issue_kv(l):
            wy(l, kv_u).start()

        def issue_q(l, u_lo):
            loop(u_lo, kv_u, lambda u: wy(l, u).start())

        def issue_o(l, t):
            for cp in oy(l, t):
                cp.start()

        def arrive(l, u):
            @pl.when(keeper)
            def _():
                wy(l, u).wait_recv()
                wc(l, u).start()

            @pl.when(giver)
            def _():
                wc(l, u).wait_recv()

        def arrive_o(l, t):
            @pl.when(keeper)
            def _():
                for cp, fw in zip(oy(l, t), oc(l, t)):
                    cp.wait_recv()
                    fw.start()

            @pl.when(giver)
            def _():
                for fw in oc(l, t):
                    fw.wait_recv()

        def load_unit(l, u, slot, half):
            near = wv.at[slot, pl.ds(pl.multiple_of(y * dh, dh), dh), half * UNIT:(half + 1) * UNIT]
            far = wv.at[slot, pl.ds(pl.multiple_of((1 - y) * dh, dh), dh), half * UNIT:(half + 1) * UNIT]

            @pl.when(keeper)
            def _():
                local(w_in.at[l, :, ucols(u)], near, ws.at[slot, half]).start()

            @pl.when(giver)
            def _():
                local(a_in.at[l, :, ucols(u)], near, ws.at[slot, half]).start()

            local(r_in.at[l, :, ucols(u)], far, ws.at[slot, 2 + half]).start()

        def wait_unit(slot, half):
            near = wv.at[slot, pl.ds(pl.multiple_of(y * dh, dh), dh), half * UNIT:(half + 1) * UNIT]
            far = wv.at[slot, pl.ds(pl.multiple_of((1 - y) * dh, dh), dh), half * UNIT:(half + 1) * UNIT]
            local(r_in.at[0, :, ucols(0)], near, ws.at[slot, half]).wait()
            local(r_in.at[0, :, ucols(0)], far, ws.at[slot, 2 + half]).wait()

        def load_o(l, src_at, src_ml, t, slot):
            local(src_at.at[l, :, tcols(t)], wv.at[slot, 0:aw], ws.at[slot, 0]).start()
            local(src_ml.at[l, :, tcols(t)], wv.at[slot, aw:kk], ws.at[slot, 1]).start()

        def load_o_near(l, t, slot):
            @pl.when(keeper)
            def _():
                load_o(l, w_at, w_ml, t, slot)

            @pl.when(giver)
            def _():
                load_o(l, a_at, a_ml, t, slot)

        def wait_o(slot):
            local(r_at.at[0, :, tcols(0)], wv.at[slot, 0:aw], ws.at[slot, 0]).wait()
            local(r_ml.at[0, :, tcols(0)], wv.at[slot, aw:kk], ws.at[slot, 1]).wait()

        def lrows(r):
            return pl.ds(pl.multiple_of(r * lnr, lnr), lnr)

        def ln_phase(kind):
            ln = kind
            srcs = [x, z_b.at[0, 0], xr.at[0, 0], yr.at[0]] if kind else [x]

            def loads(r, slot):
                return [local(s.at[lrows(r)], xin.at[slot, i], li.at[slot, i]) for i, s in enumerate(srcs)]

            def store_h(r, slot):
                return local(big.at[0, lrows(r), 0:d], h_all.at[ln, 0, lrows(r)], lh.at[slot])

            def store_o(r, slot):
                return local(hst.at[slot], hid.at[lrows(r)], lo.at[slot])

            def send(b):
                hy(ln, b).start()
                hx(ln, b).start()

            for cp in loads(0, 0):
                cp.start()

            def block(r):
                slot = lax.rem(r, 2)

                @pl.when(r + 1 < n_ln)
                def _():
                    for cp in loads(r + 1, 1 - slot):
                        cp.start()
                for cp in loads(r, slot):
                    cp.wait()
                if kind > 0:
                    @pl.when(r >= 2)
                    def _():
                        store_o(r - 2, slot).wait()

                def sub(i):
                    rs = pl.ds(pl.multiple_of(i * 32, 32), 32)
                    v = xin[slot, 0, rs, :].astype(F32)
                    if kind > 0:
                        zs = xin[slot, 1, rs, :].astype(F32) + xin[slot, 2, rs, :].astype(F32)
                        v = (v + (zs + xin[slot, 3, rs, :].astype(F32))).astype(BF)
                        hst[slot, rs, :] = v
                        v = v.astype(F32)
                    mean = jnp.sum(v, axis=-1, keepdims=True) * (1.0 / d)
                    cen = v - mean
                    var = jnp.sum(cen * cen, axis=-1, keepdims=True) * (1.0 / d)
                    out = cen * lax.rsqrt(var + EPSILON) * gv[ln, 0:1, :]
                    big[0, pl.ds(pl.multiple_of(r * lnr + i * 32, 32), 32), 0:d] = out.astype(BF)
                loop(0, lnr // 32, sub)
                if kind > 0:
                    store_o(r, slot).start()
                store_h(r, slot).start()

                @pl.when(r >= 1)
                def _():
                    store_h(r - 1, 1 - slot).wait()

                @pl.when(jnp.logical_and(r >= 2, lax.rem(r, 2) == 0))
                def _():
                    send(lax.div(r, 2) - 1)
            loop(0, n_ln, block)
            if kind > 0:
                store_o(n_ln - 2, 0).wait()
                store_o(n_ln - 1, 1).wait()
            store_h(n_ln - 1, 1).wait()
            send(n_hb - 1)

        barrier = pltpu.get_barrier_semaphore()
        for dev in (ypeer, xpeer, cpeer):
            pl.semaphore_signal(barrier, inc=1, device_id=dev, device_id_type=MESH)
        pl.semaphore_wait(barrier, 3)

        def gain_y():
            half = gv.at[:, :, pl.ds(pl.multiple_of(y * dh, dh), dh)]
            return remote(gain, half, g_s.at[0], g_r.at[0], ypeer)

        def lens_y():
            return remote(lens, lv.at[1], g_s.at[1], g_r.at[1], ypeer)

        def gain_l():
            return local(gain, gv.at[:, :, pl.ds(pl.multiple_of(y * dh, dh), dh)], lg.at[0])

        def lens_l():
            return local(lens, lv.at[0], lg.at[1])

        gain_y().start()
        lens_y().start()
        gain_l().start()
        lens_l().start()

        @pl.when(keeper)
        def _():
            for l in range(2):
                for cp in acopy(l):
                    cp.start()

        @pl.when(giver)
        def _():
            issue_kv(0)
            wy(0, 0).start()
        gain_l().wait()
        lens_l().wait()
        gain_y().wait()
        lens_y().wait()
        ln_phase(0)

        @pl.when(giver)
        def _():
            issue_q(0, 1)
            loop(0, n_gu, lambda j: issue_gu(0, j))
            loop(0, n_half, lambda t: issue_o(0, t))

        def layer(l):
            @pl.when(giver)
            def _():
                for cp in acopy(l):
                    cp.wait_recv()

            def h_load(s):
                return local(h_all.at[l, s], big.at[s, :, 0:d], hl.at[s])

            def m_store(s, j, buf):
                return local(ov.at[buf, :, 0:UNIT], m_b.at[s, :, ucols(j)], os_.at[0])

            def q_store(s, t, buf):
                return local(ov.at[buf], q_b.at[s, :, tcols(t)], os_.at[0])

            def kv_store(s, buf):
                return local(ov.at[buf, :, 0:UNIT], kvb.at[l, 0, lax.rem(s, 2), lax.div(s, 2)], os_.at[0])

            def wait_half():
                m_store(0, 0, 0).wait()

            def wait_full():
                q_store(0, 0, 0).wait()

            def arrive_gu(j):
                arrive(l, gate_u + j)
                arrive(l, up_u + j)

            def load_gu(j, slot):
                load_unit(l, gate_u + j, slot, 0)
                load_unit(l, up_u + j, slot, 1)

            def arrive_q(t):
                arrive(l, 2 * t)
                arrive(l, 2 * t + 1)

            def load_q(t, slot):
                load_unit(l, 2 * t, slot, 0)
                load_unit(l, 2 * t + 1, slot, 1)

            def load_kv(slot):
                load_unit(l, kv_u, slot, 0)

            def wait_tile(slot):
                wait_unit(slot, 0)
                wait_unit(slot, 1)

            def gu_step(s, j, slot, before, buf):
                acc = jnp.dot(big[s, :, 0:d], wv[slot, 0:d, :], preferred_element_type=F32)
                g = acc[:, :UNIT].astype(BF).astype(F32)
                u = acc[:, UNIT:].astype(BF).astype(F32)
                ov[buf, :, 0:UNIT] = (g * jax.nn.sigmoid(g) * u).astype(BF)
                before()
                m_store(s, j, buf).start()

            def q_step(s, t, slot, before, buf):
                ov[buf] = jnp.dot(big[s, :, 0:d], wv[slot, 0:d, :], preferred_element_type=F32).astype(BF)
                before()
                q_store(s, t, buf).start()

            def kv_step(s, slot, before, buf):
                ov[buf, :, 0:UNIT] = jnp.dot(big[s, :, 0:d], wv[slot, 0:d, 0:UNIT], preferred_element_type=F32).astype(BF)
                before()
                kv_store(s, buf).start()

            def nothing():
                pass

            def either(cond, yes, no):
                def go():
                    pl.when(cond)(yes)
                    pl.when(jnp.logical_not(cond))(no)
                return go

            def quarter():
                local(ov.at[0, 0:hr, 0:UNIT], m_b.at[0, 0:hr, ucols(0)], os_.at[0]).wait()

            def m_part(g, j, buf):
                return local(ov.at[buf, 0:hr, 0:UNIT], m_b.at[3, hhalf(g), ucols(j)], os_.at[0])

            def q_part(g, t, buf):
                return local(ov.at[buf, 0:hr], q_b.at[3, hhalf(g), tcols(t)], os_.at[0])

            def kv_part(g, buf):
                return local(ov.at[buf, 0:hr, 0:UNIT], kvb.at[l, 0, 1, 1, hhalf(g)], os_.at[0])

            def gu_half(g, j, slot, before, buf):
                acc = jnp.dot(big[3, hhalf(g), 0:d], wv[slot, 0:d, :], preferred_element_type=F32)
                gg = acc[:, :UNIT].astype(BF).astype(F32)
                u = acc[:, UNIT:].astype(BF).astype(F32)
                ov[buf, 0:hr, 0:UNIT] = (gg * jax.nn.sigmoid(gg) * u).astype(BF)
                before()
                m_part(g, j, buf).start()

            def unless(cond, no):
                return lambda: pl.when(jnp.logical_not(cond))(no)

            @pl.when(l == 0)
            def _():
                arrive(l, kv_u)
                load_kv(0)

            @pl.when(l == 1)
            def _():
                arrive(l, kv_u)
                load_kv(0)
                arrive_q(0)
                load_q(0, 1)
                wait_unit(0, 0)
                kv_step(0, 0, nothing, 0)

                def own_q(t):
                    slot = lax.rem(1 + t, 2)

                    @pl.when(t + 1 < n_q)
                    def _():
                        arrive_q(t + 1)
                        load_q(t + 1, 1 - slot)

                    @pl.when(t + 1 == n_q)
                    def _():
                        arrive_gu(0)
                        load_gu(0, 1 - slot)
                    wait_tile(slot)
                    q_step(0, t, slot, either(t == 0, wait_half, wait_full), slot)
                loop(0, n_q, own_q)

                def own_gu(j):
                    slot = lax.rem(1 + j, 2)

                    @pl.when(j + 1 < n_own)
                    def _():
                        arrive_gu(j + 1)
                        load_gu(j + 1, 1 - slot)
                    wait_tile(slot)
                    gu_step(0, j, slot, either(j == 0, wait_full, wait_half), slot)
                loop(0, n_own, own_gu)
                wait_half()
                load_kv(0)

            loop(0, n_hb, lambda b: hy(l, b).wait_recv())
            for g in range(2):
                hf(l, g).start()
            h_load(1).start()
            loop(0, n_hb, lambda b: hx(l, b).wait_recv())
            h_load(2).start()
            h_load(1).wait()
            h_load(2).wait()

            wait_unit(0, 0)

            def kv_a(s):
                @pl.when(s == 1)
                def _():
                    pl.when(l == 0)(lambda: arrive_q(0))
                    load_q(0, 1)
                kv_step(s, 0, unless(s == l, wait_half), s)
            loop(l, 3, kv_a)

            def q_a(t):
                slot = lax.rem(1 + t, 2)
                wait_tile(slot)

                def shard(s):
                    @pl.when(jnp.logical_and(s == 1, t + 1 < n_q))
                    def _():
                        pl.when(l == 0)(lambda: arrive_q(t + 1))
                        load_q(t + 1, 1 - slot)
                    q_step(s, t, slot, either(jnp.logical_and(t == 0, s == l), wait_half, wait_full), s)
                loop(l, 3, shard)

                @pl.when(t == 0)
                def _():
                    kvx(l, 0).start()
            loop(0, n_q, q_a)
            wait_full()

            def attend(a, middle):
                kvx(l, a).wait_recv()

                def at_loads(b, slot):
                    rs = pl.ds(pl.multiple_of(b * pos, pos), pos)

                    def at(quarter):
                        return kvv.at[slot, pl.ds(pl.multiple_of(quarter * pos, pos), pos)]
                    return (local(q_b.at[a, rs], qv.at[slot, xx], ai.at[slot, 0]),
                            local(q_b.at[2 + a, rs], qv.at[slot, 1 - xx], ai.at[slot, 1]),
                            local(kvb.at[l, 0, a, 0, rs], at(2 * xx + c), ai.at[slot, 2]),
                            local(kvb.at[l, 0, a, 1, rs], at(2 * (1 - xx) + c), ai.at[slot, 3]),
                            local(kvb.at[l, 1, a, 0, rs], at(2 * xx + 1 - c), ai.at[slot, 4]),
                            local(kvb.at[l, 1, a, 1, rs], at(2 * (1 - xx) + 1 - c), ai.at[slot, 5]))

                def o_stores(b, slot):
                    rs = pl.ds(pl.multiple_of(b * pos, pos), pos)
                    out = []
                    for blk in range(2):
                        sh = a + 2 * (blk + xx - 2 * blk * xx)
                        for i in range(n_q):
                            n = blk * n_q + i
                            out.append(local(ab.at[slot, n * pos:(n + 1) * pos], o_b.at[sh, rs, i * TILE:(i + 1) * TILE], ao.at[slot, n]))
                    return out

                for cp in at_loads(0, 0):
                    cp.start()

                def seq(b):
                    slot = lax.rem(b, 2)

                    @pl.when(b + 1 < seqs)
                    def _():
                        for cp in at_loads(b + 1, 1 - slot):
                            cp.start()
                    pl.when(b == seqs // 2)(middle)
                    for cp in at_loads(b, slot):
                        cp.wait()

                    @pl.when(b >= 2)
                    def _():
                        for cp in o_stores(b - 2, slot):
                            cp.wait()
                    for blk in range(2):
                        nk = 2 * pos * (blk + 1)
                        keys = kvv[slot, 0:nk, 0:HEAD]
                        vals = kvv[slot, 0:nk, HEAD:2 * HEAD]
                        q_all = jnp.concatenate([qv[slot, blk, :, hd * HEAD:(hd + 1) * HEAD] for hd in range(q_heads)], axis=0)
                        sv[:, 0:nk] = lax.dot_general(q_all, keys, (((1,), (1,)), ((), ())), preferred_element_type=F32)
                        for r0 in range(0, rows, SOFT):
                            rs = slice(r0, r0 + SOFT)
                            qpos = lax.broadcasted_iota(jnp.int32, (SOFT, 2 * pos), 0) + ((2 * blk + c) * pos + r0 % pos)
                            kpos = lax.broadcasted_iota(jnp.int32, (SOFT, 2 * pos), 1) + (nk - 2 * pos)
                            last = jnp.minimum(qpos, lv[a, pl.ds(b, 1), 0:2 * pos] - 1)
                            s = sv[rs, nk - 2 * pos:nk] * qscale
                            s = jnp.where(kpos <= last, s, NEG)
                            if blk:
                                s = jnp.concatenate([sv[rs, 0:2 * pos] * qscale, s], axis=1)
                            e = jnp.exp2(s - jnp.max(s, axis=-1, keepdims=True))
                            ov[0, rs, 0:nk] = (e / jnp.sum(e, axis=-1, keepdims=True)).astype(BF)
                        o = jnp.dot(ov[0, :, 0:nk], vals, preferred_element_type=F32).astype(BF)
                        per = TILE // HEAD
                        for hd in range(q_heads):
                            n = blk * n_q + hd // per
                            ab[slot, n * pos:(n + 1) * pos, (hd % per) * HEAD:(hd % per + 1) * HEAD] = o[hd * pos:(hd + 1) * pos]
                    for cp in o_stores(b, slot):
                        cp.start()
                loop(0, seqs, seq)
                for b in (seqs - 2, seqs - 1):
                    for cp in o_stores(b, b % 2):
                        cp.wait()

            def first_gu():
                pl.when(l == 0)(lambda: arrive_gu(0))
                load_gu(0, 1)
            attend(0, first_gu)

            early = early0 + (early1 - early0) * l
            late = late0 + (late1 - late0) * l

            def part(g):
                j_lo = early * g
                j_hi = early + (late - early) * g

                def gu_a(j):
                    slot = lax.rem(1 + j + g, 2)
                    s_lo = l * lax.max(1 - lax.div(j, n_own), 0)
                    wait_tile(slot)

                    def shard(s):
                        @pl.when(jnp.logical_and(s == 1, j + 1 < j_hi))
                        def _():
                            pl.when(jnp.logical_or(l == 0, j + 1 >= n_own))(lambda: arrive_gu(j + 1))
                            load_gu(j + 1, 1 - slot)

                        @pl.when(jnp.logical_and(s == 1, j + 1 == j_hi))
                        def _():
                            load_kv(1 - g)

                        def before():
                            @pl.when(jnp.logical_and(s == s_lo, g == 1))
                            def _():
                                quarter()

                            @pl.when(jnp.logical_or(s != s_lo, jnp.logical_and(g == 0, j != 0)))
                            def _():
                                wait_half()
                        gu_step(s, j, slot, before, s)
                    loop(s_lo, 3, shard)

                    @pl.when(g == 1)
                    def _():
                        gu_half(0, j, slot, wait_half, 3)
                loop(j_lo, j_hi, gu_a)

                hf(l, g).wait_recv()
                load = local(h_all.at[l, 3, hhalf(g)], big.at[3, hhalf(g), 0:d], hl.at[3])
                load.start()
                load_q(0, g)
                wait_unit(1 - g, 0)
                load.wait()
                acc = jnp.dot(big[3, hhalf(g), 0:d], wv[1 - g, 0:d, 0:UNIT], preferred_element_type=F32)
                ov[1, 0:hr, 0:UNIT] = acc.astype(BF)
                either(g == 0, wait_half, quarter)()
                kv_part(g, 1).start()

                def q_b3(t):
                    slot = lax.rem(t + g, 2)

                    @pl.when(t + 1 < n_q)
                    def _():
                        load_q(t + 1, 1 - slot)

                    @pl.when(t + 1 == n_q)
                    def _():
                        load_gu(0, 1 - slot)
                    wait_tile(slot)
                    buf = 3 - 2 * t
                    ov[buf, 0:hr] = jnp.dot(big[3, hhalf(g), 0:d], wv[slot, 0:d, :], preferred_element_type=F32).astype(BF)
                    either(t == 0, quarter, wait_half)()
                    q_part(g, t, buf).start()

                    @pl.when(jnp.logical_and(t == 0, g == 1))
                    def _():
                        kvx(l, 1).start()
                loop(0, n_q, q_b3)

                def gu_b(j):
                    slot = lax.rem(j + g, 2)

                    @pl.when(j + 1 < j_hi)
                    def _():
                        load_gu(j + 1, 1 - slot)

                    @pl.when(j + 1 == j_hi)
                    def _():
                        arrive_gu(j_hi)
                        load_gu(j_hi, 1 - slot)
                    wait_tile(slot)
                    gu_half(g, j, slot, either(j == 0, wait_half, quarter), 3 - 2 * lax.rem(j, 2))
                loop(0, j_hi * g + early * (1 - g), gu_b)
            loop(0, 2, part)
            quarter()
            def om_load(s):
                return (local(o_b.at[s], big.at[s, :, 0:aw], ol_s.at[s]), local(m_b.at[s], big.at[s, :, aw:kk], ml_s.at[s]))
            def tau(k):
                return lax.rem(y + lax.div(k, n_half), 2) * n_half + lax.rem(k, n_half)

            def z_store(s, t, buf):
                return local(ov.at[buf], z_b.at[l, s, :, tcols(t)], os_.at[0])

            def send_x(t, i):
                for h in range(2):
                    xz(l, 2 * t + h, i).start()

            @pl.when(l == 1)
            def _():
                def ahead_gu(j):
                    slot = lax.rem(1 + j, 2)

                    @pl.when(j + 1 < n_gu)
                    def _():
                        arrive_gu(j + 1)
                        load_gu(j + 1, 1 - slot)

                    @pl.when(j + 1 == n_gu)
                    def _():
                        load_o_near(l, 0, 1 - slot)
                    wait_tile(slot)
                    gu_step(2, j, slot, unless(j == late, wait_half), slot)
                loop(late, n_gu, ahead_gu)
                wait_half()
                for cp in om_load(2):
                    cp.start()
                for cp in om_load(2):
                    cp.wait()

                def ahead_out(k):
                    slot = lax.rem(1 + k, 2)

                    @pl.when(k + 1 < n_half)
                    def _():
                        load_o_near(l, k + 1, 1 - slot)

                    @pl.when(k + 1 == n_half)
                    def _():
                        load_gu(late, 1 - slot)
                    wait_o(slot)
                    ov[slot] = jnp.dot(big[2], wv[slot], preferred_element_type=F32).astype(BF)

                    @pl.when(k > 0)
                    def _():
                        z_store(2, 0, 0).wait()
                        send_x(tau(k - 1), 0)
                    z_store(2, tau(k), slot).start()
                loop(0, n_half, ahead_out)
                z_store(2, 0, 0).wait()
                send_x(tau(n_half - 1), 0)
            attend(1, nothing)

            def gu_c(j):
                slot = lax.rem(1 + j, 2)
                wait_tile(slot)

                def shard(i):
                    s = i + l * lax.div(i, 2)

                    @pl.when(jnp.logical_and(i == 1, j + 1 < n_gu))
                    def _():
                        pl.when(l == 0)(lambda: arrive_gu(j + 1))
                        load_gu(j + 1, 1 - slot)

                    @pl.when(jnp.logical_and(i == 1, j + 1 == n_gu))
                    def _():
                        load_o_near(l, 0, 1 - slot)
                    gu_step(s, j, slot, unless(jnp.logical_and(j == late, i == 0), wait_half), s)
                loop(0, 4 - l, shard)
            loop(late, n_gu, gu_c)
            wait_half()
            oslot = (n_gu + 1) % 2

            @pl.when(l == 0)
            def _():
                for cp in om_load(2):
                    cp.start()
            for s in (3, 1, 0):
                for cp in om_load(s):
                    cp.start()

            @pl.when(jnp.logical_and(giver, l == 0))
            def _():
                issue_kv(1)
                issue_q(1, 0)

            def add_tile(k):
                t = tau(k)

                def half(h):
                    w = 2 * t + h
                    xz(l, w, 0).wait_recv()
                    xz(l, w, 1).wait_recv()
                    lhs = local(z_b.at[l, 1, :, ucols(w)], ab.at[0, :, 0:UNIT], ad.at[0])
                    rhs = local(xr.at[l, 1, :, ucols(w)], ab.at[1, :, 0:UNIT], ad.at[1])
                    lhs.start()
                    rhs.start()
                    lhs.wait()
                    rhs.wait()

                    def sub(i):
                        rs = pl.ds(pl.multiple_of(i * 128, 128), 128)
                        ab[0, rs, 0:UNIT] = (ab[0, rs, 0:UNIT].astype(F32) + ab[1, rs, 0:UNIT].astype(F32)).astype(BF)
                    loop(0, rows // 128, sub)
                    out = local(ab.at[0, :, 0:UNIT], sq.at[l, :, ucols(w)], ad.at[2])
                    out.start()
                    out.wait()
                    yz(l, w).start()
                loop(0, 2, half)

                @pl.when(jnp.logical_and(jnp.logical_and(giver, l == 0), jnp.logical_or(k == 3, k == n_out - 1)))
                def _():
                    issue_gu(1, lax.div(k, n_half))

            def out_tile(k):
                slot = lax.rem(k + oslot, 2)
                t = tau(k)
                si_lo = l * (1 - lax.div(k, n_half))
                wait_o(slot)

                def order(si):
                    return si + 2 - lax.div(si, 2) * (2 * si - 1)

                def shard(si):
                    s = order(si)

                    @pl.when(jnp.logical_and(si == 2, k + 1 < n_half))
                    def _():
                        load_o_near(l, k + 1, 1 - slot)

                    @pl.when(jnp.logical_and(si == 2, jnp.logical_and(k + 1 >= n_half, k + 1 < n_out)))
                    def _():
                        arrive_o(l, k + 1 - n_half)
                        load_o(l, r_at, r_ml, k + 1 - n_half, 1 - slot)

                    @pl.when(k == 0)
                    def _():
                        for cp in om_load(s):
                            cp.wait()
                    acc = jnp.dot(big[s], wv[slot], preferred_element_type=F32)
                    ov[s] = acc.astype(BF)

                    @pl.when(jnp.logical_or(si > si_lo, k > 0))
                    def _():
                        z_store(0, t, 0).wait()

                    @pl.when(jnp.logical_and(si >= 1 + si_lo, si < 3))
                    def _():
                        send_x(t, si - 1)
                    z_store(s, t, s).start()
                loop(si_lo, 4, shard)

                @pl.when(jnp.logical_and(k >= 3, lax.rem(k, 2) == 1))
                def _():
                    done = lax.div(k - 3, 2) * (1 + l)
                    loop(done, done + 1 + l, add_tile)
            loop(0, n_out, out_tile)
            z_store(0, 0, 0).wait()

            def last_half(w):
                yz(l, w).wait_recv()
                parts = (hid.at[:, ucols(w)], z_b.at[l, 0, :, ucols(w)], xr.at[l, 0, :, ucols(w)], yr.at[l, :, ucols(w)])
                cps = [local(p, ov.at[i, :, 0:UNIT], hl.at[i]) for i, p in enumerate(parts)]
                for cp in cps:
                    cp.start()
                for cp in cps:
                    cp.wait()

                def sub(i):
                    rs = pl.ds(pl.multiple_of(i * 128, 128), 128)
                    zs = ov[1, rs, 0:UNIT].astype(F32) + ov[2, rs, 0:UNIT].astype(F32)
                    ov[0, rs, 0:UNIT] = (ov[0, rs, 0:UNIT].astype(F32) + (zs + ov[3, rs, 0:UNIT].astype(F32))).astype(BF)
                loop(0, rows // 128, sub)
                out = local(ov.at[0, :, 0:UNIT], y_out.at[:, ucols(w)], lo.at[0])
                out.start()
                out.wait()
            @pl.when(l == 0)
            def _():
                loop(3, n_out, add_tile)

            @pl.when(l == 1)
            def _():
                def last_tile(k):
                    loop(0, 2, lambda h: last_half(2 * tau(k) + h))
                loop(0, 4, lambda i: last_tile(i + 2 * lax.div(i, 2)))
                add_tile(6)
                loop(0, 2, lambda i: last_tile(2 + 4 * i))
                add_tile(7)
                loop(0, 2, lambda i: last_tile(7 - 4 * i))

            @pl.when(l == 0)
            def _():
                loop(0, 2 * n_out, lambda w: yz(l, w).wait_recv())
                ln_phase(1)

                @pl.when(giver)
                def _():
                    loop(n_own, n_gu, lambda j: issue_gu(1, j))
                    loop(0, n_half, lambda t: issue_o(1, t))


            def sent_h(b):
                hy(l, b).wait_send()
                hx(l, b).wait_send()
            loop(0, n_hb, sent_h)
            for g in range(2):
                hf(l, g).wait_send()
            for a in range(2):
                kvx(l, a).wait_send()

            def sent_z(w):
                xz(l, w, 0).wait_send()
                xz(l, w, 1).wait_send()
                yz(l, w).wait_send()
            loop(0, 2 * n_out, sent_z)

            @pl.when(giver)
            def _():
                loop(0, n_units, lambda u: wy(l, u).wait_send())

                def sent_o(t):
                    for cp in oy(l, t):
                        cp.wait_send()
                loop(0, n_half, sent_o)

            @pl.when(keeper)
            def _():
                loop(0, n_units, lambda u: wc(l, u).wait_send())

                def sent_o(t):
                    for cp in oc(l, t):
                        cp.wait_send()
                loop(0, n_half, sent_o)
                for cp in acopy(l):
                    cp.wait_send()
        loop(0, 2, layer)

    return kernel


def solution(mesh):
    batch_axes = ('rep', 'data')

    def device_step(x_loc, len_loc, gain_loc, w_in_loc, w_attn_loc, w_mlp_loc):
        seqs, pos, d = x_loc.shape
        rows = seqs * pos
        layers, dh, block_in = w_in_loc.shape
        aw = w_attn_loc.shape[1]
        ff = w_mlp_loc.shape[1]
        n_units = block_in // UNIT
        n_out = d // TILE
        kk = aw + ff
        seq_len = pos * mesh.shape['model']
        lens = jnp.broadcast_to(len_loc[:, None], (seqs, seq_len)).astype(jnp.int32)
        gain = jnp.broadcast_to(gain_loc.astype(F32)[:, None, :], (layers, 8, dh))

        def buf(*shape):
            return jax.ShapeDtypeStruct(shape, BF)

        outs = [buf(rows, d), buf(layers, dh, block_in), buf(layers, aw, dh), buf(layers, ff, dh),
                buf(layers, dh, block_in), buf(layers, aw, dh), buf(layers, ff, dh),
                buf(layers, 4, rows, d), buf(layers, 2, 2, 2, rows, 2 * HEAD), buf(4, rows, aw), buf(4, rows, ff),
                buf(layers, 4, rows, d), buf(layers, 2, rows, d), buf(layers, rows, d), buf(layers, rows, d), buf(rows, d),
                buf(4, rows, aw)]
        dma = pltpu.SemaphoreType.DMA
        n_hb = rows // 128
        scratch = [pltpu.VMEM((4, rows, kk), BF), pltpu.VMEM((2, kk, TILE), BF), pltpu.VMEM((4, rows, TILE), BF),
                   pltpu.VMEM((2, rows, TILE), BF),
                   pltpu.VMEM((2, 4, 64, d), BF), pltpu.VMEM((2, 64, d), BF), pltpu.VMEM((layers, 8, d), F32),
                   pltpu.VMEM((2, seqs, seq_len), jnp.int32), pltpu.VMEM((2, 2, pos, aw), BF),
                   pltpu.VMEM((2, seq_len, 2 * HEAD), BF), pltpu.VMEM((rows, seq_len), F32),
                   dma((layers, 3)), dma((layers, 3)),
                   dma((layers, n_units)), dma((layers, n_units)), dma((layers, n_units)), dma((layers, n_units)),
                   dma((layers, n_out // 2, 2)), dma((layers, n_out // 2, 2)),
                   dma((layers, n_out // 2, 2)), dma((layers, n_out // 2, 2)),
                   dma((layers, n_hb)), dma((layers, n_hb)), dma((layers, n_hb)), dma((layers, n_hb)),
                   dma((layers, 2)), dma((layers, 2)), dma((layers, 2)), dma((layers, 2)),
                   dma((layers, 2 * n_out, 2)), dma((layers, 2 * n_out, 2)), dma((layers, 2 * n_out)), dma((layers, 2 * n_out)),
                   dma((2,)), dma((2,)), dma((2,)), dma((2, 4)), dma((2,)), dma((2,)), dma((4,)), dma((2, 4)), dma((4,)),
                   dma((2, 6)), dma((2, 2 * (aw // TILE))), dma((4,)), dma((4,)), dma((3,))]
        hbm = pl.BlockSpec(memory_space=pl.ANY)
        kernel = make_kernel(rows, seqs, d, dh, block_in, aw, ff, n_units)
        got = pl.pallas_call(
            kernel, out_shape=outs, in_specs=[hbm] * 6, out_specs=[hbm] * len(outs), scratch_shapes=scratch, name='two_layers',
            compiler_params=pltpu.CompilerParams(collective_id=0, has_side_effects=True, vmem_limit_bytes=67_000_000),
        )(x_loc.reshape(rows, d), lens, gain, w_in_loc, w_attn_loc, w_mlp_loc)
        return got[0].reshape(seqs, pos, d)

    return jax.shard_map(device_step, mesh=mesh,
                         in_specs=(P(batch_axes, 'model', None), P(batch_axes), P(None, 'data'), P(None, 'data', 'model'),
                                   P(None, 'model', 'data'), P(None, 'model', 'data')),
                         out_specs=P(batch_axes, 'model', None), check_vma=False)
```
